128 devices in a mesh: dp: 1, ep: 64 (over z, y, x), tp: 2 (over core).
Axes of the slice: x: 4, y: 4, z: 4, core: 2. Of those that a mesh axis runs over, the one named last changes fastest.
Arguments:
- X: bfloat16 [32768, 2048], P(('dp', 'ep', 'tp'))
- idx: int32 [32768, 8], P(('dp', 'ep', 'tp'))
- g: float32 [32768, 8], P(('dp', 'ep', 'tp'))
- W1: bfloat16 [64, 2048, 1024], P('ep', None, 'tp')
- W3: bfloat16 [64, 2048, 1024], P('ep', None, 'tp')
- W2: bfloat16 [64, 1024, 2048], P('ep', 'tp')
Outputs:
- output: bfloat16 [32768, 2048], P(('dp', 'ep', 'tp'))
All inputs are finite; a program needn't handle non-finite values.
Results may differ from the reference program's by a relative error of at most 0.0107182.
Values are sent between devices in bfloat16 or wider.
A program may use at most 1 GiB of HBM per device.

```python
import jax
import jax.numpy as jnp
from jax import lax

D = 2048
F = 1024
E = 64
TOP = 8
T_LOC = 256
NDEV = 128
C = 2 * TOP * T_LOC // E
T = NDEV * T_LOC


def _weights(key, shape, fan):
    def one(k):
        return (jax.random.normal(k, shape, jnp.float32) * fan ** -0.5).astype(jnp.bfloat16)
    return lax.map(one, jax.random.split(key, E))


def setup_inputs(seed: int = 0, part: int = 0) -> dict:
    key = jax.random.PRNGKey(seed)
    kdata, kw = jax.random.split(key)
    kx, kr, kg = jax.random.split(jax.random.fold_in(kdata, part), 3)
    k1, k3, k2 = jax.random.split(kw, 3)
    x = jax.random.normal(kx, (T, D), jnp.float32).astype(jnp.bfloat16)
    expert_rank = jnp.arange(E, dtype=jnp.uint32)
    wait_scale = jnp.uint32(512) - (jnp.uint32(256) * expert_rank) // jnp.uint32(max(E - 1, 1))
    wait_time = (jax.random.bits(jax.random.fold_in(kr, 7), (T, E), jnp.uint32) >> 10) * wait_scale[None, :]
    idx = jnp.argsort(wait_time, axis=1)[:, :TOP].astype(jnp.int32)
    g = jax.random.uniform(kg, (T, TOP), jnp.float32, 0.25, 1.0)
    return {"X": x, "idx": idx, "g": g,
            "W1": _weights(k1, (D, F), D), "W3": _weights(k3, (D, F), D), "W2": _weights(k2, (F, D), F)}


def _slots(ids):
    oh = (ids[:, None] == jnp.arange(E, dtype=jnp.int32)[None, :]).astype(jnp.int32)
    return jnp.sum(oh * (jnp.cumsum(oh, axis=0) - 1), axis=1)


def reference(X, idx, g, W1, W3, W2):
    ids = idx.reshape(NDEV, T_LOC * TOP)
    s = jax.vmap(_slots)(ids)
    keep = s < C
    dest = jnp.where(keep, ids * C + s, E * C)
    xr = jnp.repeat(X.reshape(NDEV, T_LOC, D), TOP, axis=1)
    buf = jax.vmap(lambda x, dd: jnp.zeros((E * C, D), X.dtype).at[dd].set(x, mode="drop"))(xr, dest)
    buf = buf.reshape(NDEV, E, C, D).transpose(1, 0, 2, 3)

    def expert(a):
        xb, w1, w3, w2 = a

        def rows(x):
            h1 = jnp.dot(x, w1, preferred_element_type=jnp.float32)
            h3 = jnp.dot(x, w3, preferred_element_type=jnp.float32)
            h = (jax.nn.silu(h1) * h3).astype(jnp.bfloat16)
            return jnp.dot(h, w2, preferred_element_type=jnp.float32).astype(jnp.bfloat16)
        return lax.map(rows, xb)

    yb = lax.map(expert, (buf, W1, W3, W2))
    yb = yb.transpose(1, 0, 2, 3).reshape(NDEV, E * C, D)
    ysel = jax.vmap(lambda y, dd: y[jnp.minimum(dd, E * C - 1)])(yb, dest)
    wgt = jnp.where(keep, g.reshape(NDEV, T_LOC * TOP), 0.0)
    out = jnp.sum(ysel.astype(jnp.float32).reshape(NDEV, T_LOC, TOP, D) * wgt.reshape(NDEV, T_LOC, TOP, 1), axis=2)
    return out.reshape(T, D).astype(jnp.bfloat16)
```

```python
import functools

import jax
import jax.numpy as jnp
from jax import lax
from jax.experimental import pallas as pl
from jax.experimental.pallas import tpu as pltpu
from jax.sharding import PartitionSpec as P

CF = 2
N_AX = 4
AXES = 3
VMEM_LIMIT = 60 * 2**20
MESH = pl.DeviceIdType.MESH
BF = jnp.bfloat16
F32 = jnp.float32


def _coords(me):
    return [(me // N_AX**a) % N_AX for a in range(AXES)]


def _shift(m, moves):
    return sum(((m[a] + moves.get(a, 0)) % N_AX) * N_AX**a for a in range(AXES))


def _color(c):
    return (c + 1) % 3, (c + 2) % 3, c


def _barrier(m, tp):
    bar = pltpu.get_barrier_semaphore()
    for a in range(AXES):
        for d in range(1, N_AX):
            pl.semaphore_signal(bar, inc=1, device_id={"ep": _shift(m, {a: d})}, device_id_type=MESH)
    pl.semaphore_signal(bar, inc=1, device_id={"tp": 1 - tp}, device_id_type=MESH)
    pl.semaphore_wait(bar, AXES * (N_AX - 1) + 1)


def _order(k):
    return 1 + 2 * k - 3 * (k // 2)


def _dispatch_kernel(parts, cap, x_ref, idx_ref, w1_ref, w3_ref, w2_ref, rows_ref, p1_ref, p3_ref, p2_ref,
                     ag0, ag1, ag2, st0, st1, st2, meta, tri, ag_send, ag_recv, mt_send, mt_recv,
                     blk_send, blk_recv, loc_sem, w_send, w_recv):
    me, tp = lax.axis_index("ep"), lax.axis_index("tp")
    m = _coords(me)
    ags, sts = (ag0, ag1, ag2), (st0, st1, st2)
    t_loc = x_ref.shape[0]
    _barrier(m, tp)

    w_copies = [pltpu.make_async_remote_copy(s, d, w_send.at[i], w_recv.at[i], device_id={"tp": 1 - tp},
                                             device_id_type=MESH)
                for i, (s, d) in enumerate(((w1_ref, p1_ref), (w3_ref, p3_ref), (w2_ref, p2_ref)))]

    def source(c, i, own):
        off, w = parts[c]
        return (x_ref.at[:, pl.ds(off, w)], idx_ref) if own else (ags[c].at[i], meta.at[c, i])

    def row_copies(c, i_from, i_to, own, axis, d):
        src, mt = source(c, i_from, own)
        to = {"ep": _shift(m, {axis: d})}
        return (pltpu.make_async_remote_copy(src, ags[c].at[i_to], ag_send.at[c, i_to], ag_recv.at[c, i_to],
                                             device_id=to, device_id_type=MESH),
                pltpu.make_async_remote_copy(mt, meta.at[c, i_to], mt_send.at[c, i_to], mt_recv.at[c, i_to],
                                             device_id=to, device_id_type=MESH))

    def start(copies):
        for cp in reversed(copies):
            cp.start()

    def block_copy(c, i, d3):
        a1, a2, a3 = _color(c)
        off, w = parts[c]
        src = _shift(m, {a1: N_AX - i // 4, a2: N_AX - i % 4})
        part = sts[c].at[i, pl.ds(d3 * cap, cap)]
        dst = rows_ref.at[pl.ds(pl.multiple_of(src * cap, cap), cap), pl.ds(off, w)]
        if d3 == 0:
            return pltpu.make_async_copy(part, dst, loc_sem.at[c, i])
        return pltpu.make_async_remote_copy(part, dst, blk_send.at[c, i, d3 - 1], blk_recv,
                                            device_id={"ep": _shift(m, {a3: d3})}, device_id_type=MESH)

    def process(c, i, own):
        _, _, a3 = _color(c)
        off, w = parts[c]
        ids = idx_ref[...] if own else meta[c, i]
        member = [jnp.max((ids == _shift(m, {a3: d3})).astype(F32), axis=0, keepdims=True) for d3 in range(N_AX)]
        table = jnp.concatenate(member + [jnp.zeros((4, t_loc), F32)], axis=0)
        slots = jnp.dot(table.astype(BF), tri[...], preferred_element_type=F32)
        key = jnp.where(table > 0, slots, -1.0)
        want = lax.broadcasted_iota(jnp.int32, (cap, t_loc), 0).astype(F32)
        pick = jnp.concatenate([jnp.where(key[d3:d3 + 1] == want, 1.0, 0.0) for d3 in range(N_AX)], axis=0)
        xs = x_ref[:, off:off + w] if own else ags[c][i]
        sts[c][i] = jnp.dot(pick.astype(BF), xs, preferred_element_type=F32).astype(BF)
        for d3 in (1, 3, 2, 0):
            block_copy(c, i, d3).start()

    for c in range(AXES):
        a1, a2, _ = _color(c)
        for d in (1, 3, 2):
            start(row_copies(c, 0, d * 4, True, a1, d))
        for d in (1, 3, 2):
            start(row_copies(c, 0, d, True, a2, d))
    for cp in w_copies:
        cp.start()
    r = lax.broadcasted_iota(jnp.int32, (t_loc, t_loc), 0)
    q = lax.broadcasted_iota(jnp.int32, (t_loc, t_loc), 1)
    tri[...] = jnp.where(r < q, 1.0, 0.0).astype(BF)
    for c in range(AXES):
        process(c, 0, True)

    def wait_rows(c, i):
        for cp in row_copies(c, i, i, False, 0, 1):
            cp.wait_recv()

    def relay(k, carry):
        d1 = _order(k)
        for c in range(AXES):
            wait_rows(c, d1 * 4)
            for d in (1, 3, 2):
                start(row_copies(c, d1 * 4, d1 * 4 + d, False, _color(c)[1], d))
        for c in range(AXES):
            process(c, d1 * 4, False)
        return carry

    lax.fori_loop(0, 3, relay, 0)

    def rest(k, carry):
        d2, k1 = _order(k // 4), k % 4
        i = k1 * 4 + d2
        for c in range(AXES):
            wait_rows(c, i)
            process(c, i, False)
        return carry

    lax.fori_loop(0, 12, rest, 0)

    def drain(i, carry):
        for c in range(AXES):
            for d3 in range(1, N_AX):
                block_copy(c, i, d3).wait_send()
            block_copy(c, i, 0).wait()
        return carry

    lax.fori_loop(0, 16, drain, 0)

    def drain_rows(i, carry):
        for c in range(AXES):
            for cp in row_copies(c, i, i, False, 0, 1):
                cp.wait_send()
        return carry

    lax.fori_loop(1, 16, drain_rows, 0)
    for cp in w_copies:
        cp.wait()
    n_in = rows_ref.shape[0] * 3 // 4
    pltpu.make_async_copy(rows_ref.at[pl.ds(0, n_in)], rows_ref.at[pl.ds(0, n_in)], blk_recv).wait()


def _dispatch(x, idx_t, w1, w3, w2, n_exp, cap):
    t_loc, d = x.shape
    parts = ((0, d * 3 // 8), (d * 3 // 8, d * 5 // 16), (d * 11 // 16, d * 5 // 16))
    any_spec = pl.BlockSpec(memory_space=pl.ANY)
    vm = pl.BlockSpec(memory_space=pltpu.VMEM)
    dma = pltpu.SemaphoreType.DMA
    out = [jax.ShapeDtypeStruct((n_exp * cap, d), x.dtype)] + [jax.ShapeDtypeStruct(w.shape, w.dtype) for w in (w1, w3, w2)]
    return pl.pallas_call(
        functools.partial(_dispatch_kernel, parts, cap),
        out_shape=out,
        in_specs=[vm, vm, any_spec, any_spec, any_spec],
        out_specs=[any_spec] * 4,
        scratch_shapes=[pltpu.VMEM((16, t_loc, w), BF) for _, w in parts]
        + [pltpu.VMEM((16, 4 * cap, w), BF) for _, w in parts]
        + [pltpu.VMEM((3, 16) + idx_t.shape, jnp.int32), pltpu.VMEM((t_loc, t_loc), BF),
           dma((3, 16)), dma((3, 16)), dma((3, 16)), dma((3, 16)), dma((3, 16, 3)), dma, dma((3, 16)),
           dma((3,)), dma((3,))],
        compiler_params=pltpu.CompilerParams(collective_id=0, has_side_effects=True, vmem_limit_bytes=VMEM_LIMIT),
        name="dispatch",
    )(x, idx_t, w1, w3, w2)


def _expert_kernel(x_ref, w1a, w3a, w2a, w1b, w3b, w2b, y_ref):
    x = x_ref[...]
    y = None
    for w1, w3, w2 in ((w1a, w3a, w2a), (w1b, w3b, w2b)):
        a = jnp.dot(x, w1[...], preferred_element_type=F32)
        b = jnp.dot(x, w3[...], preferred_element_type=F32)
        h = (jax.nn.silu(a) * b).astype(BF)
        part = jnp.dot(h, w2[...], preferred_element_type=F32)
        y = part if y is None else y + part
    y_ref[...] = y.astype(BF)


def _experts(rows, w1a, w3a, w2a, w1b, w3b, w2b):
    n, d = rows.shape
    f = w1a.shape[1]
    blk = 256
    wide = pl.BlockSpec((d, f), lambda i: (0, 0), pipeline_mode=pl.Buffered(1))
    tall = pl.BlockSpec((f, d), lambda i: (0, 0), pipeline_mode=pl.Buffered(1))
    return pl.pallas_call(
        _expert_kernel,
        out_shape=jax.ShapeDtypeStruct((n, d), BF),
        grid=(n // blk,),
        in_specs=[pl.BlockSpec((blk, d), lambda i: (i, 0)), wide, wide, tall, wide, wide, tall],
        out_specs=pl.BlockSpec((blk, d), lambda i: (i, 0)),
        compiler_params=pltpu.CompilerParams(vmem_limit_bytes=VMEM_LIMIT),
        cost_estimate=pl.CostEstimate(flops=12 * n * d * f, bytes_accessed=4 * n * d + 12 * d * f, transcendentals=2 * n * f),
        name="experts",
    )(rows, w1a, w3a, w2a, w1b, w3b, w2b)


def _split3(v):
    hi = v.astype(BF)
    r = v - hi.astype(F32)
    mid = r.astype(BF)
    return hi, mid, (r - mid.astype(F32)).astype(BF)


def _combine_kernel(cap, idx_ref, g_ref, back_ref, y_ref, key, gates, acc):
    t_loc, top = idx_ref.shape
    n_exp = key.shape[1]
    i = pl.program_id(0)

    @pl.when(i == 0)
    def _():
        e = lax.broadcasted_iota(jnp.int32, (t_loc, n_exp), 1)
        member = jnp.zeros((t_loc, n_exp), F32)
        gate = jnp.zeros((t_loc, n_exp), F32)
        for j in range(top):
            hit = idx_ref[:, j:j + 1] == e
            member = jnp.where(hit, 1.0, member)
            gate = jnp.where(hit, g_ref[:, j:j + 1], gate)
        r = lax.broadcasted_iota(jnp.int32, (t_loc, t_loc), 0)
        q = lax.broadcasted_iota(jnp.int32, (t_loc, t_loc), 1)
        lower = jnp.where(q < r, 1.0, 0.0).astype(BF)
        slots = jnp.dot(lower, member.astype(BF), preferred_element_type=F32)
        key[...] = jnp.where(member > 0, slots, -1.0).astype(BF)
        for k, part in enumerate(_split3(gate)):
            gates[k] = part
        acc[...] = jnp.zeros_like(acc)

    wide = back_ref.shape[0]
    e = lax.broadcasted_iota(jnp.int32, (n_exp, wide), 0)
    col = lax.broadcasted_iota(jnp.int32, (n_exp, wide), 1)
    spread = jnp.where(e == i * (wide // cap) + col // cap, 1.0, 0.0).astype(BF)
    slot = (lax.broadcasted_iota(jnp.int32, (t_loc, wide), 1) % cap).astype(F32)
    hit = jnp.dot(key[...], spread, preferred_element_type=F32) == slot
    total = acc[...]
    for k in range(3):
        weight = jnp.where(hit, jnp.dot(gates[k], spread, preferred_element_type=F32), 0.0).astype(BF)
        total += jnp.dot(weight, back_ref[...], preferred_element_type=F32)
    acc[...] = total

    @pl.when(i == pl.num_programs(0) - 1)
    def _():
        y_ref[...] = acc[...].astype(BF)


def _combine(idx, g, back, n_exp, cap):
    t_loc, top = idx.shape
    d = back.shape[1]
    blk = 256
    return pl.pallas_call(
        functools.partial(_combine_kernel, cap),
        out_shape=jax.ShapeDtypeStruct((t_loc, d), BF),
        grid=(back.shape[0] // blk,),
        in_specs=[pl.BlockSpec((t_loc, top), lambda i: (0, 0)), pl.BlockSpec((t_loc, top), lambda i: (0, 0)),
                  pl.BlockSpec((blk, d), lambda i: (i, 0))],
        out_specs=pl.BlockSpec((t_loc, d), lambda i: (0, 0)),
        scratch_shapes=[pltpu.VMEM((t_loc, n_exp), BF), pltpu.VMEM((3, t_loc, n_exp), BF), pltpu.VMEM((t_loc, d), F32)],
        compiler_params=pltpu.CompilerParams(vmem_limit_bytes=VMEM_LIMIT),
        name="combine",
    )(idx, g, back)


def solution(mesh):
    ep = mesh.shape["ep"]
    rows = P(("dp", "ep", "tp"), None)

    def local(x, idx, g, w1, w3, w2):
        t_loc, d = x.shape
        top = idx.shape[1]
        cap = CF * top * t_loc // ep
        w1, w3, w2 = w1[0], w3[0], w2[0]
        xe, w1b, w3b, w2b = _dispatch(x, idx.T, w1, w3, w2, ep, cap)
        y = _experts(xe, w1, w3, w2, w1b, w3b, w2b)
        back = lax.all_to_all(y.reshape(ep, cap, d), "ep", 0, 0, tiled=True).reshape(ep * cap, d)
        return _combine(idx, g, back, ep, cap)

    return jax.shard_map(local, mesh=mesh,
                         in_specs=(rows, rows, rows, P("ep", None, "tp"), P("ep", None, "tp"), P("ep", "tp", None)),
                         out_specs=rows, check_vma=False)
```

```python
import functools

import jax
import jax.numpy as jnp
from jax import lax
from jax.experimental import pallas as pl
from jax.experimental.pallas import tpu as pltpu
from jax.sharding import PartitionSpec as P

CF = 2
N_AX = 4
AXES = 3
VMEM_LIMIT = 60 * 2**20
MESH = pl.DeviceIdType.MESH
BF = jnp.bfloat16
F32 = jnp.float32


def _coords(me):
    return [(me // N_AX**a) % N_AX for a in range(AXES)]


def _shift(m, moves):
    return sum(((m[a] + moves.get(a, 0)) % N_AX) * N_AX**a for a in range(AXES))


def _color(c):
    return (c + 1) % 3, (c + 2) % 3, c


def _barrier(m, tp):
    bar = pltpu.get_barrier_semaphore()
    for a in range(AXES):
        for d in range(1, N_AX):
            pl.semaphore_signal(bar, inc=1, device_id={"ep": _shift(m, {a: d})}, device_id_type=MESH)
    pl.semaphore_signal(bar, inc=1, device_id={"tp": 1 - tp}, device_id_type=MESH)
    pl.semaphore_wait(bar, AXES * (N_AX - 1) + 1)


def _order(k):
    return 1 + 2 * k - 3 * (k // 2)


def _dispatch_kernel(parts, cap, x_ref, idx_ref, w1_ref, w3_ref, w2_ref, rows_ref, p1_ref, p3_ref, p2_ref,
                     ag0, ag1, ag2, st0, st1, st2, meta, tri, ag_send, ag_recv, mt_send, mt_recv,
                     blk_send, blk_recv, loc_sem, w_send, w_recv):
    me, tp = lax.axis_index("ep"), lax.axis_index("tp")
    m = _coords(me)
    ags, sts = (ag0, ag1, ag2), (st0, st1, st2)
    t_loc = x_ref.shape[0]
    _barrier(m, tp)

    w_copies = [pltpu.make_async_remote_copy(s, d, w_send.at[i], w_recv.at[i], device_id={"tp": 1 - tp},
                                             device_id_type=MESH)
                for i, (s, d) in enumerate(((w1_ref, p1_ref), (w3_ref, p3_ref), (w2_ref, p2_ref)))]

    def source(c, i, own):
        off, w = parts[c]
        return (x_ref.at[:, pl.ds(off, w)], idx_ref) if own else (ags[c].at[i], meta.at[c, i])

    def row_copies(c, i_from, i_to, own, axis, d):
        src, mt = source(c, i_from, own)
        to = {"ep": _shift(m, {axis: d})}
        return (pltpu.make_async_remote_copy(src, ags[c].at[i_to], ag_send.at[c, i_to], ag_recv.at[c, i_to],
                                             device_id=to, device_id_type=MESH),
                pltpu.make_async_remote_copy(mt, meta.at[c, i_to], mt_send.at[c, i_to], mt_recv.at[c, i_to],
                                             device_id=to, device_id_type=MESH))

    def start(copies):
        for cp in reversed(copies):
            cp.start()

    def block_copy(c, i, d3):
        a1, a2, a3 = _color(c)
        off, w = parts[c]
        src = (i // 4) * N_AX**a1 + (i % 4) * N_AX**a2 + d3 * N_AX**a3
        part = sts[c].at[i, pl.ds(d3 * cap, cap)]
        dst = rows_ref.at[pl.ds(pl.multiple_of(src * cap, cap), cap), pl.ds(off, w)]
        if d3 == 0:
            return pltpu.make_async_copy(part, dst, loc_sem.at[c, i])
        return pltpu.make_async_remote_copy(part, dst, blk_send.at[c, i, d3 - 1], blk_recv,
                                            device_id={"ep": _shift(m, {a3: d3})}, device_id_type=MESH)

    def process(c, i, own):
        _, _, a3 = _color(c)
        off, w = parts[c]
        ids = idx_ref[...] if own else meta[c, i]
        member = [jnp.max((ids == _shift(m, {a3: d3})).astype(F32), axis=0, keepdims=True) for d3 in range(N_AX)]
        table = jnp.concatenate(member + [jnp.zeros((4, t_loc), F32)], axis=0)
        slots = jnp.dot(table.astype(BF), tri[...], preferred_element_type=F32)
        key = jnp.where(table > 0, slots, -1.0)
        want = lax.broadcasted_iota(jnp.int32, (cap, t_loc), 0).astype(F32)
        pick = jnp.concatenate([jnp.where(key[d3:d3 + 1] == want, 1.0, 0.0) for d3 in range(N_AX)], axis=0)
        xs = x_ref[:, off:off + w] if own else ags[c][i]
        sts[c][i] = jnp.dot(pick.astype(BF), xs, preferred_element_type=F32).astype(BF)
        for d3 in (1, 3, 2, 0):
            block_copy(c, i, d3).start()

    for c in range(AXES):
        a1, a2, _ = _color(c)
        for d in (1, 3, 2):
            start(row_copies(c, 0, d * 4, True, a1, d))
        for d in (1, 3, 2):
            start(row_copies(c, 0, d, True, a2, d))
    for cp in w_copies:
        cp.start()
    r = lax.broadcasted_iota(jnp.int32, (t_loc, t_loc), 0)
    q = lax.broadcasted_iota(jnp.int32, (t_loc, t_loc), 1)
    tri[...] = jnp.where(r < q, 1.0, 0.0).astype(BF)
    for c in range(AXES):
        process(c, 0, True)

    def wait_rows(c, i):
        for cp in row_copies(c, i, i, False, 0, 1):
            cp.wait_recv()

    def relay(k, carry):
        d1 = _order(k)
        for c in range(AXES):
            wait_rows(c, d1 * 4)
            for d in (1, 3, 2):
                start(row_copies(c, d1 * 4, d1 * 4 + d, False, _color(c)[1], d))
        for c in range(AXES):
            process(c, d1 * 4, False)
        return carry

    lax.fori_loop(0, 3, relay, 0)

    def rest(k, carry):
        d2, k1 = _order(k // 4), k % 4
        i = k1 * 4 + d2
        for c in range(AXES):
            wait_rows(c, i)
            process(c, i, False)
        return carry

    lax.fori_loop(0, 12, rest, 0)

    def drain(i, carry):
        for c in range(AXES):
            for d3 in range(1, N_AX):
                block_copy(c, i, d3).wait_send()
            block_copy(c, i, 0).wait()
        return carry

    lax.fori_loop(0, 16, drain, 0)

    def drain_rows(i, carry):
        for c in range(AXES):
            for cp in row_copies(c, i, i, False, 0, 1):
                cp.wait_send()
        return carry

    lax.fori_loop(1, 16, drain_rows, 0)
    for cp in w_copies:
        cp.wait()
    n_in = rows_ref.shape[0] * 3 // 4
    pltpu.make_async_copy(rows_ref.at[pl.ds(0, n_in)], rows_ref.at[pl.ds(0, n_in)], blk_recv).wait()


def _dispatch(x, idx_t, w1, w3, w2, n_exp, cap):
    t_loc, d = x.shape
    parts = _parts(d)
    any_spec = pl.BlockSpec(memory_space=pl.ANY)
    vm = pl.BlockSpec(memory_space=pltpu.VMEM)
    dma = pltpu.SemaphoreType.DMA
    out = [jax.ShapeDtypeStruct((n_exp * cap, d), x.dtype)] + [jax.ShapeDtypeStruct(w.shape, w.dtype) for w in (w1, w3, w2)]
    return pl.pallas_call(
        functools.partial(_dispatch_kernel, parts, cap),
        out_shape=out,
        in_specs=[vm, vm, any_spec, any_spec, any_spec],
        out_specs=[any_spec] * 4,
        scratch_shapes=[pltpu.VMEM((16, t_loc, w), BF) for _, w in parts]
        + [pltpu.VMEM((16, 4 * cap, w), BF) for _, w in parts]
        + [pltpu.VMEM((3, 16) + idx_t.shape, jnp.int32), pltpu.VMEM((t_loc, t_loc), BF),
           dma((3, 16)), dma((3, 16)), dma((3, 16)), dma((3, 16)), dma((3, 16, 3)), dma, dma((3, 16)),
           dma((3,)), dma((3,))],
        compiler_params=pltpu.CompilerParams(collective_id=0, has_side_effects=True, vmem_limit_bytes=VMEM_LIMIT),
        name="dispatch",
    )(x, idx_t, w1, w3, w2)


def _split3(v):
    hi = v.astype(BF)
    r = v - hi.astype(F32)
    mid = r.astype(BF)
    return hi, mid, (r - mid.astype(F32)).astype(BF)


def _pack(idx_ref, g_ref, n_exp):
    t_loc, top = idx_ref.shape
    e = lax.broadcasted_iota(jnp.int32, (t_loc, n_exp), 1)
    member = jnp.zeros((t_loc, n_exp), F32)
    gate = jnp.zeros((t_loc, n_exp), F32)
    for j in range(top):
        hit = idx_ref[:, j:j + 1] == e
        member = jnp.where(hit, 1.0, member)
        gate = jnp.where(hit, g_ref[:, j:j + 1], gate)
    r = lax.broadcasted_iota(jnp.int32, (t_loc, t_loc), 0)
    q = lax.broadcasted_iota(jnp.int32, (t_loc, t_loc), 1)
    lower = jnp.where(q < r, 1.0, 0.0).astype(BF)
    slots = jnp.dot(lower, member.astype(BF), preferred_element_type=F32)
    key = jnp.where(member > 0, slots, -1.0).astype(BF)
    return jnp.concatenate((key,) + _split3(gate), axis=1)


def _far(d):
    return N_AX - d


def _order4(k):
    return (1 + 2 * k - 3 * (k // 2)) % N_AX


def _return_kernel(parts, cap, ring_n, rows_ref, idx_ref, g_ref, w1a, w3a, w2a, w1b, w3b, w2b, y_ref,
                   ra0, ra1, ra2, rb0, rb1, rb2, cr0, cr1, cr2, packs, mine, *sems):
    (x_sem, w_sem, a_send, a_recv, b_send, b_recv, c_send, c_recv, p_send, p_recv) = sems
    me, tp = lax.axis_index("ep"), lax.axis_index("tp")
    m = _coords(me)
    ra, rb, cr = (ra0, ra1, ra2), (rb0, rb1, rb2), (cr0, cr1, cr2)
    d, f = w1a.shape
    t_loc = idx_ref.shape[0]
    n_exp = N_AX**AXES
    blk = N_AX * cap
    groups = rows_ref.shape[0] // blk
    _barrier(m, tp)
    weights = (w1a, w3a, w2a, w1b, w3b, w2b)

    def p_copy(c, d1):
        return pltpu.make_async_remote_copy(mine, packs.at[c, d1 - 1], p_send.at[c, d1 - 1], p_recv.at[c, d1 - 1],
                                            device_id={"ep": _shift(m, {_color(c)[0]: d1})}, device_id_type=MESH)

    def a_wait(c, i):
        three = ra[c].at[i, pl.ds(0, 3 * cap)]
        pltpu.make_async_copy(three, three, a_recv.at[c, i]).wait()

    def b_copy(c, d1, d2):
        i = d1 * 4 + d2
        return pltpu.make_async_remote_copy(ra[c].at[i], rb[c].at[d1, d2 - 1], b_send.at[c, i], b_recv.at[c, i],
                                            device_id={"ep": _shift(m, {_color(c)[1]: _far(d2)})}, device_id_type=MESH)

    def forward(k, carry):
        d1, d2 = _order4(k // 4), k % 4
        for c in range(AXES):
            a_wait(c, d1 * 4 + d2)

            @pl.when(d2 > 0)
            def _():
                b_copy(c, d1, d2).start()
        return carry

    def compute(wv1a, wv3a, wv2a, wv1b, wv3b, wv2b, xbuf, ring):
        vmem = (wv1a, wv3a, wv2a, wv1b, wv3b, wv2b)
        w_copies = [pltpu.make_async_copy(s, v, w_sem.at[i]) for i, (s, v) in enumerate(zip(weights, vmem))]

        def x_copy(k):
            return pltpu.make_async_copy(rows_ref.at[pl.ds(k * blk, blk)], xbuf.at[k % 2], x_sem.at[k % 2])

        x_copy(0).start()
        for cp in w_copies:
            cp.start()
        mine[...] = _pack(idx_ref, g_ref, n_exp)
        for c in range(AXES):
            for d1 in (1, 3, 2):
                p_copy(c, d1).start()
        for cp in w_copies:
            cp.wait()

        def a_each(k, remote, local):
            dy, dz = k % 4, k // 4
            for c in range(AXES):
                a1, a2, a3 = _color(c)
                off, w = parts[c]
                for dx in range(N_AX):
                    at = (dx, dy, dz)
                    i, d3 = at[a1] * 4 + at[a2], at[a3]

                    def far(c=c, dx=dx, i=i, d3=d3, off=off, w=w, a3=a3):
                        remote(pltpu.make_async_remote_copy(
                            ring.at[k % ring_n, pl.ds(dx * cap, cap), pl.ds(off, w)],
                            ra[c].at[i, pl.ds(d3 * cap, cap)], a_send.at[k % ring_n, c * 4 + dx], a_recv.at[c, i],
                            device_id={"ep": _shift(m, {a3: _far(d3)})}, device_id_type=MESH))

                    if c == 0:
                        far() if dx else local(c, dx, i)
                    else:
                        pl.when(d3 > 0)(far)
                        pl.when(d3 == 0)(lambda c=c, dx=dx, i=i: local(c, dx, i))

        def step(k, carry):
            x_copy(k).wait()

            @pl.when(k + 1 < groups)
            def _():
                x_copy(k + 1).start()

            @pl.when(k >= ring_n)
            def _():
                a_each(k - ring_n, lambda cp: cp.wait_send(), lambda c, dx, i: None)

            x = xbuf[k % 2]
            y = None
            for w1, w3, w2 in ((wv1a, wv3a, wv2a), (wv1b, wv3b, wv2b)):
                a = jnp.dot(x, w1[...], preferred_element_type=F32)
                b = jnp.dot(x, w3[...], preferred_element_type=F32)
                h = (jax.nn.silu(a) * b).astype(BF)
                part = jnp.dot(h, w2[...], preferred_element_type=F32)
                y = part if y is None else y + part
            ring[k % ring_n] = y.astype(BF)

            def keep(c, dx, i):
                off, w = parts[c]
                ra[c][i, 0:cap, :] = ring[k % ring_n, dx * cap:(dx + 1) * cap, off:off + w]

            a_each(k, lambda cp: cp.start(), keep)
            return carry

        lax.fori_loop(0, groups, step, 0)
        lax.fori_loop(0, groups, forward, 0)

        def drain(k, carry):
            a_each(k, lambda cp: cp.wait_send(), lambda c, dx, i: None)
            return carry

        lax.fori_loop(groups - ring_n, groups, drain, 0)

    pl.run_scoped(compute, *[pltpu.VMEM(w.shape, BF) for w in weights], pltpu.VMEM((2, blk, d), BF),
                  pltpu.VMEM((ring_n, blk, d), BF))

    def combine(acc, cs0, cs1, cs2):
        cs = (cs0, cs1, cs2)

        def partial_sum(c, d1, own):
            _, a2, a3 = _color(c)
            off, w = parts[c]
            table = mine[...] if own else packs[c, d1 - 1]
            row = lax.broadcasted_iota(jnp.int32, (N_AX * n_exp, blk), 0)
            col = lax.broadcasted_iota(jnp.int32, (N_AX * n_exp, blk), 1)
            slot = (lax.broadcasted_iota(jnp.int32, (t_loc, blk), 1) % cap).astype(F32)
            total = None
            for d2 in range(N_AX):
                base = _shift(m, {a2: d2}) - m[a3] * N_AX**a3
                e = base + ((m[a3] + col // cap) % N_AX) * N_AX**a3
                spread = [jnp.where(row == e + n_exp * k, 1.0, 0.0).astype(BF) for k in range(4)]
                hit = jnp.dot(table, spread[0], preferred_element_type=F32) == slot
                data = ra[c][d1 * 4] if d2 == 0 else rb[c][d1, d2 - 1]
                for k in range(1, 4):
                    gate = jnp.dot(table, spread[k], preferred_element_type=F32)
                    part = jnp.dot(jnp.where(hit, gate, 0.0).astype(BF), data, preferred_element_type=F32)
                    total = part if total is None else total + part
            return total

        def b_wait(c, d1):
            for d2 in range(1, N_AX):
                b_copy(c, d1, d2).wait_recv()

        def c_copy(c, d1):
            return pltpu.make_async_remote_copy(cs[c].at[d1 - 1], cr[c].at[d1 - 1], c_send.at[c, d1 - 1],
                                                c_recv.at[c, d1 - 1],
                                                device_id={"ep": _shift(m, {_color(c)[0]: _far(d1)})},
                                                device_id_type=MESH)

        for c in range(AXES):
            for d1 in range(1, N_AX):
                p_copy(c, d1).wait_recv()

        def send(k, carry):
            d1 = _order(k)
            for c in range(AXES):
                b_wait(c, d1)
                cs[c][d1 - 1] = partial_sum(c, d1, False)
                c_copy(c, d1).start()
            return carry

        lax.fori_loop(0, N_AX - 1, send, 0)
        for c in range(AXES):
            off, w = parts[c]
            b_wait(c, 0)
            acc[:, off:off + w] = partial_sum(c, 0, True)
        for c in range(AXES):
            off, w = parts[c]
            for d1 in range(1, N_AX):
                c_copy(c, d1).wait()
            y_ref[:, off:off + w] = (acc[:, off:off + w] + cr[c][0] + cr[c][1] + cr[c][2]).astype(BF)

    pl.run_scoped(combine, pltpu.VMEM((t_loc, d), F32), *[pltpu.VMEM((3, t_loc, w), F32) for _, w in parts])

    def drain_b(k, carry):
        for c in range(AXES):
            for d2 in range(1, N_AX):
                b_copy(c, k, d2).wait_send()
        return carry

    lax.fori_loop(0, N_AX, drain_b, 0)
    for c in range(AXES):
        for d1 in range(1, N_AX):
            p_copy(c, d1).wait_send()


def _parts(d):
    return (0, d * 3 // 8), (d * 3 // 8, d * 5 // 16), (d * 11 // 16, d * 5 // 16)


def _return(rows, idx, g, weights, cap):
    n, d = rows.shape
    t_loc = idx.shape[0]
    parts = _parts(d)
    blk = N_AX * cap
    ring_n = 6
    any_spec = pl.BlockSpec(memory_space=pl.ANY)
    vm = pl.BlockSpec(memory_space=pltpu.VMEM)
    dma = pltpu.SemaphoreType.DMA
    return pl.pallas_call(
        functools.partial(_return_kernel, parts, cap, ring_n),
        out_shape=jax.ShapeDtypeStruct((t_loc, d), BF),
        in_specs=[any_spec, vm, vm] + [any_spec] * 6,
        out_specs=vm,
        scratch_shapes=[pltpu.VMEM((16, blk, w), BF) for _, w in parts]
        + [pltpu.VMEM((N_AX, 3, blk, w), BF) for _, w in parts]
        + [pltpu.VMEM((3, t_loc, w), F32) for _, w in parts]
        + [pltpu.VMEM((3, 3, t_loc, 4 * N_AX**AXES), BF), pltpu.VMEM((t_loc, 4 * N_AX**AXES), BF),
           dma((2,)), dma((6,)), dma((ring_n, 12)), dma((3, 16)), dma((3, 16)), dma((3, 16)), dma((3, 3)), dma((3, 3)),
           dma((3, 3)), dma((3, 3))],
        compiler_params=pltpu.CompilerParams(collective_id=1, has_side_effects=True, vmem_limit_bytes=63 * 2**20),
        name="experts_return",
    )(rows, idx, g, *weights)


def solution(mesh):
    ep = mesh.shape["ep"]
    rows = P(("dp", "ep", "tp"), None)

    def local(x, idx, g, w1, w3, w2):
        t_loc, d = x.shape
        top = idx.shape[1]
        cap = CF * top * t_loc // ep
        w1, w3, w2 = w1[0], w3[0], w2[0]
        xe, w1b, w3b, w2b = _dispatch(x, idx.T, w1, w3, w2, ep, cap)
        return _return(xe, idx, g, (w1, w3, w2, w1b, w3b, w2b), cap)

    return jax.shard_map(local, mesh=mesh,
                         in_specs=(rows, rows, rows, P("ep", None, "tp"), P("ep", None, "tp"), P("ep", "tp", None)),
                         out_specs=rows, check_vma=False)
```

```python
import functools

import jax
import jax.numpy as jnp
from jax import lax
from jax.experimental import pallas as pl
from jax.experimental.pallas import tpu as pltpu
from jax.sharding import PartitionSpec as P

CF = 2
N_AX = 4
AXES = 3
VMEM_LIMIT = 60 * 2**20
MESH = pl.DeviceIdType.MESH
BF = jnp.bfloat16
F32 = jnp.float32


def _coords(me):
    return [(me // N_AX**a) % N_AX for a in range(AXES)]


def _shift(m, moves):
    return sum(((m[a] + moves.get(a, 0)) % N_AX) * N_AX**a for a in range(AXES))


def _color(c):
    return (c + 1) % 3, (c + 2) % 3, c


def _greet(m, tp):
    bar = pltpu.get_barrier_semaphore()
    for a in range(AXES):
        for d in range(1, N_AX):
            pl.semaphore_signal(bar, inc=1, device_id={"ep": _shift(m, {a: d})}, device_id_type=MESH)
    pl.semaphore_signal(bar, inc=1, device_id={"tp": 1 - tp}, device_id_type=MESH)


def _meet():
    pl.semaphore_wait(pltpu.get_barrier_semaphore(), AXES * (N_AX - 1) + 1)


def _line(k):
    return k + k // 2 - 2 * (k // 3)


def _order(k):
    return 1 + 2 * k - 3 * (k // 2)


def _dispatch_kernel(parts, cap, x_ref, idx_ref, w1_ref, w3_ref, w2_ref, rows_ref, p1_ref, p3_ref, p2_ref,
                     ag0, ag1, ag2, st0, st1, st2, meta, tri, ag_send, ag_send2, ag_recv, mt_send, mt_recv,
                     blk_send, blk_recv, loc_sem, w_send, w_recv):
    me, tp = lax.axis_index("ep"), lax.axis_index("tp")
    m = _coords(me)
    ags, sts = (ag0, ag1, ag2), (st0, st1, st2)
    t_loc = x_ref.shape[0]
    half = t_loc // 2
    _greet(m, tp)

    w_copies = [pltpu.make_async_remote_copy(s, d, w_send.at[i], w_recv.at[i], device_id={"tp": 1 - tp},
                                             device_id_type=MESH)
                for i, (s, d) in enumerate(((w1_ref, p1_ref), (w3_ref, p3_ref), (w2_ref, p2_ref)))]

    def remote(src, dst, send, recv, axis, d):
        return pltpu.make_async_remote_copy(src, dst, send, recv, device_id={"ep": _shift(m, {axis: d})},
                                            device_id_type=MESH)

    def whole(c, i_from, i_to, own, axis, d):
        off, w = parts[c]
        src = x_ref.at[:, pl.ds(off, w)] if own else ags[c].at[i_from]
        return remote(src, ags[c].at[i_to], ag_send.at[c, i_to], ag_recv.at[c, i_to], axis, d)

    def top(c, i_from, i_to, axis):
        rows = pl.ds(0, half)
        return remote(ags[c].at[i_from, rows], ags[c].at[i_to, rows], ag_send.at[c, i_to], ag_recv.at[c, i_to], axis, 1)

    def bottom(c, i_from, i_to, axis):
        rows = pl.ds(half, half)
        return remote(ags[c].at[i_from, rows], ags[c].at[i_to, rows], ag_send2.at[c, i_to], ag_recv.at[c, i_to], axis, 3)

    def ids_copy(c, i_from, i_to, own, axis, d):
        src = idx_ref if own else meta.at[c, i_from]
        return remote(src, meta.at[c, i_to], mt_send.at[c, i_to], mt_recv.at[c, i_to], axis, d)

    def spread(c, i, step, own, axis):
        for d in (1, 3, 2):
            ids_copy(c, i, i + d * step, own, axis, d).start()
        for d in (1, 3):
            whole(c, i, i + d * step, own, axis, d).start()

    def block_copy(c, i, d3):
        a1, a2, a3 = _color(c)
        off, w = parts[c]
        src = (i // 4) * N_AX**a1 + (i % 4) * N_AX**a2 + d3 * N_AX**a3
        part = sts[c].at[i, pl.ds(d3 * cap, cap)]
        dst = rows_ref.at[pl.ds(pl.multiple_of(src * cap, cap), cap), pl.ds(off, w)]
        if d3 == 0:
            return pltpu.make_async_copy(part, dst, loc_sem.at[c, i])
        return pltpu.make_async_remote_copy(part, dst, blk_send.at[c, i, d3 - 1], blk_recv,
                                            device_id={"ep": _shift(m, {a3: d3})}, device_id_type=MESH)

    def pick(c, i, own):
        _, _, a3 = _color(c)
        off, w = parts[c]
        ids = idx_ref[...] if own else meta[c, i]
        member = [jnp.max((ids == _shift(m, {a3: d3})).astype(F32), axis=0, keepdims=True) for d3 in range(N_AX)]
        table = jnp.concatenate(member + [jnp.zeros((4, t_loc), F32)], axis=0)
        slots = jnp.dot(table.astype(BF), tri[...], preferred_element_type=F32)
        key = jnp.where(table > 0, slots, -1.0)
        want = lax.broadcasted_iota(jnp.int32, (cap, t_loc), 0).astype(F32)
        one_hot = jnp.concatenate([jnp.where(key[d3:d3 + 1] == want, 1.0, 0.0) for d3 in range(N_AX)], axis=0)
        xs = x_ref[:, off:off + w] if own else ags[c][i]
        sts[c][i] = jnp.dot(one_hot.astype(BF), xs, preferred_element_type=F32).astype(BF)

    def send_blocks(c, i):
        for d3 in (1, 3, 2, 0):
            block_copy(c, i, d3).start()

    def process(i):
        for c in range(AXES):
            pick(c, i, False)
            send_blocks(c, i)

    def wait_rows(c, i):
        ids_copy(c, i, i, False, 0, 1).wait_recv()
        whole(c, i, i, False, 0, 1).wait_recv()

    r = lax.broadcasted_iota(jnp.int32, (t_loc, t_loc), 0)
    q = lax.broadcasted_iota(jnp.int32, (t_loc, t_loc), 1)
    tri[...] = jnp.where(r < q, 1.0, 0.0).astype(BF)
    _meet()
    for c in range(AXES):
        a1, a2, _ = _color(c)
        spread(c, 0, 4, True, a1)
        spread(c, 0, 1, True, a2)
    for cp in w_copies:
        cp.start()
    for c in range(AXES):
        pick(c, 0, True)
        send_blocks(c, 0)

    def pass_on(c, d, i, i_to, axis):
        pl.when(d == 1)(lambda: top(c, i, i_to, axis).start())
        pl.when(d == 3)(lambda: bottom(c, i, i_to, axis).start())

    def first_near(k, carry):
        d1 = 1 + 2 * k
        for c in range(AXES):
            a1, a2, _ = _color(c)
            wait_rows(c, d1 * 4)
            pass_on(c, d1, d1 * 4, 8, a1)
            spread(c, d1 * 4, 1, False, a2)
        process(d1 * 4)
        return carry

    def second_near(k, carry):
        j, d2 = k // 2, 1 + 2 * (k % 2)
        d1 = _line(j)
        for c in range(AXES):
            wait_rows(c, d1 * 4 + d2)
            pass_on(c, d2, d1 * 4 + d2, d1 * 4 + 2, _color(c)[1])
        process(d1 * 4 + d2)
        return carry

    def second_far(k, carry):
        d1 = _line(k)
        for c in range(AXES):
            wait_rows(c, d1 * 4 + 2)
        process(d1 * 4 + 2)
        return carry

    lax.fori_loop(0, 2, first_near, 0)
    lax.fori_loop(0, 2, second_near, 0)
    for c in range(AXES):
        wait_rows(c, 8)
        spread(c, 8, 1, False, _color(c)[1])
    process(8)
    lax.fori_loop(2, 8, second_near, 0)
    lax.fori_loop(0, 4, second_far, 0)

    def drain(i, carry):
        for c in range(AXES):
            for d3 in range(1, N_AX):
                block_copy(c, i, d3).wait_send()
            block_copy(c, i, 0).wait()
        return carry

    lax.fori_loop(0, 16, drain, 0)

    def drain_far(c, i):
        top(c, i, i, 0).wait_send()
        bottom(c, i, i, 0).wait_send()

    def drain_line(d1, carry):
        for c in range(AXES):
            for d2 in range(1, N_AX):
                ids_copy(c, 0, d1 * 4 + d2, False, 0, 1).wait_send()
            for d2 in (1, 3):
                whole(c, 0, d1 * 4 + d2, False, 0, 1).wait_send()
            drain_far(c, d1 * 4 + 2)
        return carry

    lax.fori_loop(0, N_AX, drain_line, 0)
    for c in range(AXES):
        for d1 in range(1, N_AX):
            ids_copy(c, 0, d1 * 4, False, 0, 1).wait_send()
        for d1 in (1, 3):
            whole(c, 0, d1 * 4, False, 0, 1).wait_send()
        drain_far(c, 8)
    for cp in w_copies:
        cp.wait()
    n_in = rows_ref.shape[0] * 3 // 4
    pltpu.make_async_copy(rows_ref.at[pl.ds(0, n_in)], rows_ref.at[pl.ds(0, n_in)], blk_recv).wait()


def _dispatch(x, idx_t, w1, w3, w2, n_exp, cap):
    t_loc, d = x.shape
    parts = _parts(d)
    any_spec = pl.BlockSpec(memory_space=pl.ANY)
    vm = pl.BlockSpec(memory_space=pltpu.VMEM)
    dma = pltpu.SemaphoreType.DMA
    out = [jax.ShapeDtypeStruct((n_exp * cap, d), x.dtype)] + [jax.ShapeDtypeStruct(w.shape, w.dtype) for w in (w1, w3, w2)]
    return pl.pallas_call(
        functools.partial(_dispatch_kernel, parts, cap),
        out_shape=out,
        in_specs=[vm, vm, any_spec, any_spec, any_spec],
        out_specs=[any_spec] * 4,
        scratch_shapes=[pltpu.VMEM((16, t_loc, w), BF) for _, w in parts]
        + [pltpu.VMEM((16, 4 * cap, w), BF) for _, w in parts]
        + [pltpu.VMEM((3, 16) + idx_t.shape, jnp.int32), pltpu.VMEM((t_loc, t_loc), BF),
           dma((3, 16)), dma((3, 16)), dma((3, 16)), dma((3, 16)), dma((3, 16)), dma((3, 16, 3)), dma, dma((3, 16)),
           dma((3,)), dma((3,))],
        compiler_params=pltpu.CompilerParams(collective_id=0, has_side_effects=True, vmem_limit_bytes=VMEM_LIMIT),
        name="dispatch",
    )(x, idx_t, w1, w3, w2)


def _split3(v):
    hi = v.astype(BF)
    r = v - hi.astype(F32)
    mid = r.astype(BF)
    return hi, mid, (r - mid.astype(F32)).astype(BF)


def _pack(idx_ref, g_ref, n_exp):
    top, t_loc = idx_ref.shape
    idx, g = idx_ref[...].T, g_ref[...].T
    e = lax.broadcasted_iota(jnp.int32, (t_loc, n_exp), 1)
    member = jnp.zeros((t_loc, n_exp), F32)
    gate = jnp.zeros((t_loc, n_exp), F32)
    for j in range(top):
        hit = idx[:, j:j + 1] == e
        member = jnp.where(hit, 1.0, member)
        gate = jnp.where(hit, g[:, j:j + 1], gate)
    r = lax.broadcasted_iota(jnp.int32, (t_loc, t_loc), 0)
    q = lax.broadcasted_iota(jnp.int32, (t_loc, t_loc), 1)
    lower = jnp.where(q < r, 1.0, 0.0).astype(BF)
    slots = jnp.dot(lower, member.astype(BF), preferred_element_type=F32)
    key = jnp.where(member > 0, slots, -1.0).astype(BF)
    return jnp.concatenate((key,) + _split3(gate), axis=1)


def _far(d):
    return N_AX - d


def _order4(k):
    return (1 + 2 * k - 3 * (k // 2)) % N_AX


def _return_kernel(parts, cap, ring_n, rows_ref, idx_ref, g_ref, w1a, w3a, w2a, w1b, w3b, w2b, y_ref,
                   ra0, ra1, ra2, rb0, rb1, rb2, cr0, cr1, cr2, packs, mine, *sems):
    (x_sem, w_sem, a_send, a_recv, b_send, b_recv, c_send, c_recv, p_send, p_recv) = sems
    me, tp = lax.axis_index("ep"), lax.axis_index("tp")
    m = _coords(me)
    ra, rb, cr = (ra0, ra1, ra2), (rb0, rb1, rb2), (cr0, cr1, cr2)
    d, f = w1a.shape
    t_loc = idx_ref.shape[1]
    n_exp = N_AX**AXES
    blk = N_AX * cap
    groups = rows_ref.shape[0] // blk
    _greet(m, tp)
    weights = (w1a, w3a, w2a, w1b, w3b, w2b)

    def p_copy(c, d1):
        return pltpu.make_async_remote_copy(mine, packs.at[c, d1 - 1], p_send.at[c, d1 - 1], p_recv.at[c, d1 - 1],
                                            device_id={"ep": _shift(m, {_color(c)[0]: d1})}, device_id_type=MESH)

    def a_wait(c, i):
        three = ra[c].at[i, pl.ds(0, 3 * cap)]
        pltpu.make_async_copy(three, three, a_recv.at[c, i]).wait()

    def b_copy(c, d1, d2):
        i = d1 * 4 + d2
        return pltpu.make_async_remote_copy(ra[c].at[i], rb[c].at[d1, d2 - 1], b_send.at[c, i], b_recv.at[c, i],
                                            device_id={"ep": _shift(m, {_color(c)[1]: _far(d2)})}, device_id_type=MESH)

    def forward(k, carry):
        d1, d2 = _order4(k // 4), k % 4
        for c in range(AXES):
            a_wait(c, d1 * 4 + d2)

            @pl.when(d2 > 0)
            def _():
                b_copy(c, d1, d2).start()
        return carry

    def compute(wv1a, wv3a, wv2a, wv1b, wv3b, wv2b, xbuf, ring):
        vmem = (wv1a, wv3a, wv2a, wv1b, wv3b, wv2b)
        w_copies = [pltpu.make_async_copy(s, v, w_sem.at[i]) for i, (s, v) in enumerate(zip(weights, vmem))]

        def x_copy(k):
            return pltpu.make_async_copy(rows_ref.at[pl.ds(k * blk, blk)], xbuf.at[k % 2], x_sem.at[k % 2])

        x_copy(0).start()
        for cp in w_copies:
            cp.start()
        mine[...] = _pack(idx_ref, g_ref, n_exp)
        _meet()
        for c in range(AXES):
            for d1 in (1, 3, 2):
                p_copy(c, d1).start()
        for cp in w_copies:
            cp.wait()

        def a_each(k, remote, local):
            dy, dz = k % 4, k // 4
            for c in range(AXES):
                a1, a2, a3 = _color(c)
                off, w = parts[c]
                for dx in range(N_AX):
                    at = (dx, dy, dz)
                    i, d3 = at[a1] * 4 + at[a2], at[a3]

                    def far(c=c, dx=dx, i=i, d3=d3, off=off, w=w, a3=a3):
                        remote(pltpu.make_async_remote_copy(
                            ring.at[k % ring_n, pl.ds(dx * cap, cap), pl.ds(off, w)],
                            ra[c].at[i, pl.ds(d3 * cap, cap)], a_send.at[k % ring_n, c * 4 + dx], a_recv.at[c, i],
                            device_id={"ep": _shift(m, {a3: _far(d3)})}, device_id_type=MESH))

                    if c == 0:
                        far() if dx else local(c, dx, i)
                    else:
                        pl.when(d3 > 0)(far)
                        pl.when(d3 == 0)(lambda c=c, dx=dx, i=i: local(c, dx, i))

        def step(k, carry):
            x_copy(k).wait()

            @pl.when(k + 1 < groups)
            def _():
                x_copy(k + 1).start()

            @pl.when(k >= ring_n)
            def _():
                a_each(k - ring_n, lambda cp: cp.wait_send(), lambda c, dx, i: None)

            x = xbuf[k % 2]
            y = None
            for w1, w3, w2 in ((wv1a, wv3a, wv2a), (wv1b, wv3b, wv2b)):
                a = jnp.dot(x, w1[...], preferred_element_type=F32)
                b = jnp.dot(x, w3[...], preferred_element_type=F32)
                h = (jax.nn.silu(a) * b).astype(BF)
                part = jnp.dot(h, w2[...], preferred_element_type=F32)
                y = part if y is None else y + part
            ring[k % ring_n] = y.astype(BF)

            def keep(c, dx, i):
                off, w = parts[c]
                ra[c][i, 0:cap, :] = ring[k % ring_n, dx * cap:(dx + 1) * cap, off:off + w]

            a_each(k, lambda cp: cp.start(), keep)
            return carry

        lax.fori_loop(0, groups, step, 0)
        lax.fori_loop(0, groups, forward, 0)

        def drain(k, carry):
            a_each(k, lambda cp: cp.wait_send(), lambda c, dx, i: None)
            return carry

        lax.fori_loop(groups - ring_n, groups, drain, 0)

    pl.run_scoped(compute, *[pltpu.VMEM(w.shape, BF) for w in weights], pltpu.VMEM((2, blk, d), BF),
                  pltpu.VMEM((ring_n, blk, d), BF))

    def combine(acc, cs0, cs1, cs2):
        cs = (cs0, cs1, cs2)

        def partial_sum(c, d1, own):
            _, a2, a3 = _color(c)
            off, w = parts[c]
            table = mine[...] if own else packs[c, d1 - 1]
            row = lax.broadcasted_iota(jnp.int32, (N_AX * n_exp, blk), 0)
            col = lax.broadcasted_iota(jnp.int32, (N_AX * n_exp, blk), 1)
            slot = (lax.broadcasted_iota(jnp.int32, (t_loc, blk), 1) % cap).astype(F32)
            total = None
            for d2 in range(N_AX):
                base = _shift(m, {a2: d2}) - m[a3] * N_AX**a3
                e = base + ((m[a3] + col // cap) % N_AX) * N_AX**a3
                spread = [jnp.where(row == e + n_exp * k, 1.0, 0.0).astype(BF) for k in range(4)]
                hit = jnp.dot(table, spread[0], preferred_element_type=F32) == slot
                data = ra[c][d1 * 4] if d2 == 0 else rb[c][d1, d2 - 1]
                for k in range(1, 4):
                    gate = jnp.dot(table, spread[k], preferred_element_type=F32)
                    part = jnp.dot(jnp.where(hit, gate, 0.0).astype(BF), data, preferred_element_type=F32)
                    total = part if total is None else total + part
            return total

        def b_wait(c, d1):
            for d2 in range(1, N_AX):
                b_copy(c, d1, d2).wait_recv()

        def c_copy(c, d1):
            return pltpu.make_async_remote_copy(cs[c].at[d1 - 1], cr[c].at[d1 - 1], c_send.at[c, d1 - 1],
                                                c_recv.at[c, d1 - 1],
                                                device_id={"ep": _shift(m, {_color(c)[0]: _far(d1)})},
                                                device_id_type=MESH)

        for c in range(AXES):
            for d1 in range(1, N_AX):
                p_copy(c, d1).wait_recv()

        def send(k, carry):
            d1 = _order(k)
            for c in range(AXES):
                b_wait(c, d1)
                cs[c][d1 - 1] = partial_sum(c, d1, False)
                c_copy(c, d1).start()
            return carry

        lax.fori_loop(0, N_AX - 1, send, 0)
        for c in range(AXES):
            off, w = parts[c]
            b_wait(c, 0)
            acc[:, off:off + w] = partial_sum(c, 0, True)
        for c in range(AXES):
            off, w = parts[c]
            for d1 in range(1, N_AX):
                c_copy(c, d1).wait()
            y_ref[:, off:off + w] = (acc[:, off:off + w] + cr[c][0] + cr[c][1] + cr[c][2]).astype(BF)

    pl.run_scoped(combine, pltpu.VMEM((t_loc, d), F32), *[pltpu.VMEM((3, t_loc, w), F32) for _, w in parts])

    def drain_b(k, carry):
        for c in range(AXES):
            for d2 in range(1, N_AX):
                b_copy(c, k, d2).wait_send()
        return carry

    lax.fori_loop(0, N_AX, drain_b, 0)
    for c in range(AXES):
        for d1 in range(1, N_AX):
            p_copy(c, d1).wait_send()


def _parts(d):
    return (0, d * 3 // 8), (d * 3 // 8, d * 5 // 16), (d * 11 // 16, d * 5 // 16)


def _return(rows, idx, g, weights, cap):
    n, d = rows.shape
    t_loc = idx.shape[1]
    parts = _parts(d)
    blk = N_AX * cap
    ring_n = 6
    any_spec = pl.BlockSpec(memory_space=pl.ANY)
    vm = pl.BlockSpec(memory_space=pltpu.VMEM)
    dma = pltpu.SemaphoreType.DMA
    return pl.pallas_call(
        functools.partial(_return_kernel, parts, cap, ring_n),
        out_shape=jax.ShapeDtypeStruct((t_loc, d), BF),
        in_specs=[any_spec, vm, vm] + [any_spec] * 6,
        out_specs=vm,
        scratch_shapes=[pltpu.VMEM((16, blk, w), BF) for _, w in parts]
        + [pltpu.VMEM((N_AX, 3, blk, w), BF) for _, w in parts]
        + [pltpu.VMEM((3, t_loc, w), F32) for _, w in parts]
        + [pltpu.VMEM((3, 3, t_loc, 4 * N_AX**AXES), BF), pltpu.VMEM((t_loc, 4 * N_AX**AXES), BF),
           dma((2,)), dma((6,)), dma((ring_n, 12)), dma((3, 16)), dma((3, 16)), dma((3, 16)), dma((3, 3)), dma((3, 3)),
           dma((3, 3)), dma((3, 3))],
        compiler_params=pltpu.CompilerParams(collective_id=1, has_side_effects=True, vmem_limit_bytes=63 * 2**20),
        name="experts_return",
    )(rows, idx, g, *weights)


def solution(mesh):
    ep = mesh.shape["ep"]
    rows = P(("dp", "ep", "tp"), None)

    def local(x, idx, g, w1, w3, w2):
        t_loc, d = x.shape
        top = idx.shape[1]
        cap = CF * top * t_loc // ep
        w1, w3, w2 = w1[0], w3[0], w2[0]
        xe, w1b, w3b, w2b = _dispatch(x, idx.T, w1, w3, w2, ep, cap)
        return _return(xe, idx.T, g.T, (w1, w3, w2, w1b, w3b, w2b), cap)

    return jax.shard_map(local, mesh=mesh,
                         in_specs=(rows, rows, rows, P("ep", None, "tp"), P("ep", None, "tp"), P("ep", "tp", None)),
                         out_specs=rows, check_vma=False)
```

```python
import functools

import jax
import jax.numpy as jnp
from jax import lax
from jax.experimental import pallas as pl
from jax.experimental.pallas import tpu as pltpu
from jax.sharding import PartitionSpec as P

CF = 2
N_AX = 4
AXES = 3
VMEM_LIMIT = 60 * 2**20
MESH = pl.DeviceIdType.MESH
BF = jnp.bfloat16
F32 = jnp.float32


def _coords(me):
    return [(me // N_AX**a) % N_AX for a in range(AXES)]


def _shift(m, moves):
    return sum(((m[a] + moves.get(a, 0)) % N_AX) * N_AX**a for a in range(AXES))


def _color(c):
    return (c + 1) % 3, (c + 2) % 3, c


def _greet(m, tp):
    bar = pltpu.get_barrier_semaphore()
    for a in range(AXES):
        for d in range(1, N_AX):
            pl.semaphore_signal(bar, inc=1, device_id={"ep": _shift(m, {a: d})}, device_id_type=MESH)
    pl.semaphore_signal(bar, inc=1, device_id={"tp": 1 - tp}, device_id_type=MESH)


def _meet():
    pl.semaphore_wait(pltpu.get_barrier_semaphore(), AXES * (N_AX - 1) + 1)


def _line(k):
    return k + k // 2 - 2 * (k // 3)


def _order(k):
    return 1 + 2 * k - 3 * (k // 2)


def _split3(v):
    hi = v.astype(BF)
    r = v - hi.astype(F32)
    mid = r.astype(BF)
    return hi, mid, (r - mid.astype(F32)).astype(BF)


def _pack(idx_ref, g_ref, n_exp):
    top, t_loc = idx_ref.shape
    idx, g = idx_ref[...].T, g_ref[...].T
    e = lax.broadcasted_iota(jnp.int32, (t_loc, n_exp), 1)
    member = jnp.zeros((t_loc, n_exp), F32)
    gate = jnp.zeros((t_loc, n_exp), F32)
    for j in range(top):
        hit = idx[:, j:j + 1] == e
        member = jnp.where(hit, 1.0, member)
        gate = jnp.where(hit, g[:, j:j + 1], gate)
    r = lax.broadcasted_iota(jnp.int32, (t_loc, t_loc), 0)
    q = lax.broadcasted_iota(jnp.int32, (t_loc, t_loc), 1)
    lower = jnp.where(q < r, 1.0, 0.0).astype(BF)
    slots = jnp.dot(lower, member.astype(BF), preferred_element_type=F32)
    key = jnp.where(member > 0, slots, -1.0).astype(BF)
    return jnp.concatenate((key,) + _split3(gate), axis=1)


def _far(d):
    return N_AX - d


def _order4(k):
    return (1 + 2 * k - 3 * (k // 2)) % N_AX


def _parts(d):
    return (0, d * 3 // 8), (d * 3 // 8, d * 5 // 16), (d * 11 // 16, d * 5 // 16)


def _layer_kernel(parts, cap, ring_n, st_n, x_ref, idx_ref, g_ref, w1_ref, w3_ref, w2_ref, y_ref, rows_ref, cr0, cr1, cr2,
                  ag0, ag1, ag2, ra0, ra1, ra2, wp1, wp3, wp2, meta, packs, mine, tri, *sems):
    (ag_send, ag_send2, ag_recv, mt_send, mt_recv, blk_send, blk_recv, loc_sem, w_send, w_recv, w_loc, x_sem, a_send, a_recv,
     b_send, b_recv, c_send, c_recv, cr_sem, p_send, p_recv, free_sem) = sems
    me, tp = lax.axis_index("ep"), lax.axis_index("tp")
    m = _coords(me)
    ags, ra, cr = (ag0, ag1, ag2), (ra0, ra1, ra2), (cr0, cr1, cr2)
    t_loc, d = x_ref.shape
    n_exp = N_AX**AXES
    half = t_loc // 2
    blk = N_AX * cap
    groups = rows_ref.shape[0] // blk
    _greet(m, tp)

    def remote(src, dst, send, recv, axis, dist):
        return pltpu.make_async_remote_copy(src, dst, send, recv, device_id={"ep": _shift(m, {axis: dist})},
                                            device_id_type=MESH)

    w_refs, w_parts = (w1_ref, w3_ref, w2_ref), (wp1, wp3, wp2)
    w_swaps = [pltpu.make_async_remote_copy(w_refs[i], w_parts[i], w_send.at[i], w_recv.at[i], device_id={"tp": 1 - tp},
                                            device_id_type=MESH) for i in range(3)]


    def whole(c, i_from, i_to, own, axis, dist):
        off, w = parts[c]
        src = x_ref.at[:, pl.ds(off, w)] if own else ags[c].at[i_from]
        return remote(src, ags[c].at[i_to], ag_send.at[c, i_to], ag_recv.at[c, i_to], axis, dist)

    def top(c, i_from, i_to, axis):
        rows = pl.ds(0, half)
        return remote(ags[c].at[i_from, rows], ags[c].at[i_to, rows], ag_send.at[c, i_to], ag_recv.at[c, i_to], axis, 1)

    def bottom(c, i_from, i_to, axis):
        rows = pl.ds(half, half)
        return remote(ags[c].at[i_from, rows], ags[c].at[i_to, rows], ag_send2.at[c, i_to], ag_recv.at[c, i_to], axis, 3)

    def ids_copy(c, i_from, i_to, own, axis, dist):
        src = idx_ref if own else meta.at[c, i_from]
        return remote(src, meta.at[c, i_to], mt_send.at[c, i_to], mt_recv.at[c, i_to], axis, dist)

    def spread(c, i, step, own, axis):
        for dist in (1, 3, 2):
            ids_copy(c, i, i + dist * step, own, axis, dist).start()
        for dist in (1, 3):
            whole(c, i, i + dist * step, own, axis, dist).start()

    def pass_on(c, dist, i, i_to, axis):
        pl.when(dist == 1)(lambda: top(c, i, i_to, axis).start())
        pl.when(dist == 3)(lambda: bottom(c, i, i_to, axis).start())

    def wait_rows(c, i):
        ids_copy(c, i, i, False, 0, 1).wait_recv()
        whole(c, i, i, False, 0, 1).wait_recv()


    def p_copy(c, d1):
        return remote(mine, packs.at[c, d1 - 1], p_send.at[c, d1 - 1], p_recv.at[c, d1 - 1], _color(c)[0], d1)

    def a_wait(c, i):
        three = ra[c].at[i, pl.ds(0, 3 * cap)]
        pltpu.make_async_copy(three, three, a_recv.at[c, i]).wait()

    def b_copy(c, d1, d2):
        i = d1 * 4 + d2
        return remote(ra[c].at[i], ags[c].at[i], b_send.at[c, i], b_recv.at[c, i], _color(c)[1], _far(d2))

    def forward(k, carry):
        d1, d2 = _order4(k // 4), k % 4
        for c in range(AXES):
            a_wait(c, d1 * 4 + d2)

            @pl.when(d2 > 0)
            def _():
                b_copy(c, d1, d2).start()
        return carry

    def main(st0, st1, st2, wo1, wo3, wo2, xbuf, ring):
        sts, w_own = (st0, st1, st2), (wo1, wo3, wo2)
        w_loads = [pltpu.make_async_copy(w_refs[i], w_own[i], w_loc.at[i]) for i in range(3)]

        def block_copy(c, i, pos, d3):
            off, w = parts[c]
            a1, a2, a3 = _color(c)
            at = [0, 0, 0]
            at[a1], at[a2], at[a3] = i // 4, i % 4, d3
            part = sts[c].at[pos % st_n, pl.ds(d3 * cap, cap)]
            src = at[0] + N_AX * at[1] + N_AX**2 * at[2]
            dst = rows_ref.at[pl.ds(pl.multiple_of(src * cap, cap), cap), pl.ds(off, w)]
            if d3 == 0:
                return pltpu.make_async_copy(part, dst, loc_sem.at[c, pos % st_n])
            return remote(part, dst, blk_send.at[c, pos % st_n, d3 - 1], blk_recv.at[c, at[1] + N_AX * at[2]], a3, d3)

        def pick(c, i, pos, own):
            _, _, a3 = _color(c)
            off, w = parts[c]
            ids = idx_ref[...] if own else meta[c, i]
            member = [jnp.max((ids == _shift(m, {a3: d3})).astype(F32), axis=0, keepdims=True) for d3 in range(N_AX)]
            table = jnp.concatenate(member + [jnp.zeros((4, t_loc), F32)], axis=0)
            slots = jnp.dot(table.astype(BF), tri[...], preferred_element_type=F32)
            key = jnp.where(table > 0, slots, -1.0)
            want = lax.broadcasted_iota(jnp.int32, (cap, t_loc), 0).astype(F32)
            one_hot = jnp.concatenate([jnp.where(key[d3:d3 + 1] == want, 1.0, 0.0) for d3 in range(N_AX)], axis=0)
            one_hot = one_hot.astype(BF)
            for lo in range(0, w, 256):
                hi = min(lo + 256, w)
                xs = x_ref[:, off + lo:off + hi] if own else ags[c][i, :, lo:hi]
                sts[c][pos % st_n, :, lo:hi] = jnp.dot(one_hot, xs, preferred_element_type=F32).astype(BF)

        def local_wait(pos):
            for c in range(AXES):
                block_copy(c, 0, pos, 0).wait()

        def sent_wait(pos):
            for c in range(AXES):
                for d3 in range(1, N_AX):
                    block_copy(c, 0, pos, d3).wait_send()

        def process(i, pos, own=False):
            pl.when(pos >= st_n)(lambda: sent_wait(pos))
            for c in range(AXES):
                pick(c, i, pos, own)
                for d3 in (1, 3, 2, 0):
                    block_copy(c, i, pos, d3).start()
            pl.when(pos >= 1)(lambda: local_wait(pos + st_n - 1))

        r = lax.broadcasted_iota(jnp.int32, (t_loc, t_loc), 0)
        q = lax.broadcasted_iota(jnp.int32, (t_loc, t_loc), 1)
        tri[...] = jnp.where(r < q, 1.0, 0.0).astype(BF)
        for cp in w_loads:
            cp.start()
        _meet()
        for c in range(AXES):
            a1, a2, _ = _color(c)
            spread(c, 0, 4, True, a1)
            spread(c, 0, 1, True, a2)
        for cp in w_swaps:
            cp.start()
        process(0, 0, True)
        mine[...] = _pack(idx_ref, g_ref, n_exp)

        def first_near(k, carry):
            d1 = 1 + 2 * k
            for c in range(AXES):
                a1, a2, _ = _color(c)
                wait_rows(c, d1 * 4)
                pass_on(c, d1, d1 * 4, 8, a1)
                spread(c, d1 * 4, 1, False, a2)
            process(d1 * 4, 1 + k)
            return carry

        def second_near(k, carry):
            d1, d2 = _line(k // 2), 1 + 2 * (k % 2)
            for c in range(AXES):
                wait_rows(c, d1 * 4 + d2)
                pass_on(c, d2, d1 * 4 + d2, d1 * 4 + 2, _color(c)[1])
            process(d1 * 4 + d2, 3 + k + (k + 6) // 8)
            return carry

        def second_far(k, carry):
            d1 = _line(k)
            for c in range(AXES):
                wait_rows(c, d1 * 4 + 2)
            process(d1 * 4 + 2, 12 + k)
            return carry

        lax.fori_loop(0, 2, first_near, 0)
        lax.fori_loop(0, 2, second_near, 0)
        for c in range(AXES):
            wait_rows(c, 8)
            spread(c, 8, 1, False, _color(c)[1])
        process(8, 5)
        lax.fori_loop(2, 8, second_near, 0)
        for c in range(AXES):
            for d1 in (1, 3, 2):
                p_copy(c, d1).start()

        def group_of(n):
            late = n // 12
            near = n % 3
            return (1 - late) * (near + near // 2) + 2 * late, _line((1 - late) * (n // 3) + late * (n - 12))

        def x_copy(n):
            dy, dz = group_of(n)
            return pltpu.make_async_copy(rows_ref.at[pl.ds((dy + N_AX * dz) * blk, blk)], xbuf.at[n % 2], x_sem.at[n % 2])

        def rows_in(n):
            dy, dz = group_of(n)
            g = dy + N_AX * dz

            def arrived(c, count):
                off, w = parts[c]
                ref = rows_ref.at[pl.ds(g * blk, count * cap), pl.ds(off, w)]
                pltpu.make_async_copy(ref, ref, blk_recv.at[c, g]).wait()

            arrived(0, 3)
            pl.when(dy > 0)(lambda: arrived(1, 4))
            pl.when(dz > 0)(lambda: arrived(2, 4))
            x_copy(n).start()

        def a_each(n, far, near):
            dy, dz = group_of(n)
            for c in range(AXES):
                a1, a2, a3 = _color(c)
                off, w = parts[c]
                for dx in range(N_AX):
                    at = (dx, dy, dz)
                    i, d3 = at[a1] * 4 + at[a2], at[a3]

                    def go(c=c, dx=dx, i=i, d3=d3, off=off, w=w, a3=a3):
                        far(remote(ring.at[n % ring_n, pl.ds(dx * cap, cap), pl.ds(off, w)],
                                   ra[c].at[i, pl.ds(d3 * cap, cap)], a_send.at[n % ring_n, c * 4 + dx],
                                   a_recv.at[c, i], a3, _far(d3)))

                    if c == 0:
                        go() if dx else near(c, dx, i)
                    else:
                        pl.when(d3 > 0)(go)
                        pl.when(d3 == 0)(lambda c=c, dx=dx, i=i: near(c, dx, i))

        def step(n, carry):
            x_copy(n).wait()
            pl.when(n + 1 < groups)(lambda: rows_in(n + 1))

            @pl.when(n >= ring_n)
            def _():
                a_each(n - ring_n, lambda cp: cp.wait_send(), lambda c, dx, i: None)

            x = xbuf[n % 2]
            hs = []
            for w1, w3, _ in (w_own, w_parts):
                a = jnp.dot(x, w1[...], preferred_element_type=F32)
                b = jnp.dot(x, w3[...], preferred_element_type=F32)
                hs.append((jax.nn.silu(a) * b).astype(BF))
            for lo in range(0, d, 512):
                y = sum(jnp.dot(h, w[2][:, lo:lo + 512], preferred_element_type=F32) for h, w in zip(hs, (w_own, w_parts)))
                ring[n % ring_n, :, lo:lo + 512] = y.astype(BF)

            def keep(c, dx, i):
                off, w = parts[c]
                ra[c][i, 0:cap, :] = ring[n % ring_n, dx * cap:(dx + 1) * cap, off:off + w]

            a_each(n, lambda cp: cp.start(), keep)
            return carry

        lax.fori_loop(0, N_AX, second_far, 0)
        local_wait(15)
        for cp in w_loads:
            cp.wait()
        for cp in w_swaps:
            cp.wait_recv()
        rows_in(0)

        def drain_far(c, i):
            top(c, i, i, 0).wait_send()
            bottom(c, i, i, 0).wait_send()

        def drain_line(d1, carry):
            for c in range(AXES):
                for d2 in range(1, N_AX):
                    ids_copy(c, 0, d1 * 4 + d2, False, 0, 1).wait_send()
                for d2 in (1, 3):
                    whole(c, 0, d1 * 4 + d2, False, 0, 1).wait_send()
                drain_far(c, d1 * 4 + 2)
            return carry

        lax.fori_loop(0, N_AX, drain_line, 0)
        for c in range(AXES):
            for d1 in range(1, N_AX):
                ids_copy(c, 0, d1 * 4, False, 0, 1).wait_send()
            for d1 in (1, 3):
                whole(c, 0, d1 * 4, False, 0, 1).wait_send()
            drain_far(c, 8)
        for a in range(AXES):
            for dist in range(1, N_AX):
                pl.semaphore_signal(free_sem, inc=1, device_id={"ep": _shift(m, {a: dist})}, device_id_type=MESH)

        lax.fori_loop(0, groups, step, 0)
        pl.semaphore_wait(free_sem, AXES * (N_AX - 1))
        lax.fori_loop(0, groups, forward, 0)

        def drain_ring(n, carry):
            a_each(n, lambda cp: cp.wait_send(), lambda c, dx, i: None)
            return carry

        lax.fori_loop(groups - ring_n, groups, drain_ring, 0)
        for pos in range(16 - st_n, 16):
            sent_wait(pos)
        for cp in w_swaps:
            cp.wait_send()

    weight_scratch = [pltpu.VMEM(w.shape, BF) for w in w_refs]
    pl.run_scoped(main, *[pltpu.VMEM((st_n, blk, w), BF) for _, w in parts], *weight_scratch, pltpu.VMEM((2, blk, d), BF),
                  pltpu.VMEM((ring_n, blk, d), BF))

    def combine(acc, yv, cs0, cs1, cs2, cv0, cv1, cv2):
        cs, cv = (cs0, cs1, cs2), (cv0, cv1, cv2)

        def add_sum(c, d1, d2, own, data):
            _, a2, a3 = _color(c)
            off, w = parts[c]
            table = mine[...] if own else packs[c, d1 - 1]
            row = lax.broadcasted_iota(jnp.int32, (N_AX * n_exp, blk), 0)
            col = lax.broadcasted_iota(jnp.int32, (N_AX * n_exp, blk), 1)
            slot = (lax.broadcasted_iota(jnp.int32, (t_loc, blk), 1) % cap).astype(F32)
            e = _shift(m, {a2: d2}) - m[a3] * N_AX**a3 + ((m[a3] + col // cap) % N_AX) * N_AX**a3
            wide = [jnp.where(row == e + n_exp * k, 1.0, 0.0).astype(BF) for k in range(4)]
            hit = jnp.dot(table, wide[0], preferred_element_type=F32) == slot
            gates = [jnp.where(hit, jnp.dot(table, wide[k], preferred_element_type=F32), 0.0).astype(BF) for k in (1, 2, 3)]
            for lo in range(0, w, 256):
                hi = min(lo + 256, w)
                rows = data[:, lo:hi]
                v = sum(jnp.dot(gate, rows, preferred_element_type=F32) for gate in gates)
                at = acc.at[:, off + lo:off + hi] if own else cs[c].at[d1 - 1, :, lo:hi]
                at[...] = v if data_first(d2) else at[...] + v

        def data_first(d2):
            return isinstance(d2, int)

        def partial_sum(c, d1, own):
            add_sum(c, d1, 0, own, ra[c].at[d1 * 4])

            def more(d2, carry):
                b_copy(c, d1, d2).wait_recv()
                add_sum(c, d1, d2, own, ags[c].at[d1 * 4 + d2])
                return carry

            lax.fori_loop(1, N_AX, more, 0)

        def c_copy(c, d1):
            return remote(cs[c].at[d1 - 1], cr[c].at[d1 - 1], c_send.at[c, d1 - 1], c_recv.at[c, d1 - 1], _color(c)[0],
                          _far(d1))

        for c in range(AXES):
            for d1 in range(1, N_AX):
                p_copy(c, d1).wait_recv()

        def send(k, carry):
            d1 = _order(k)
            for c in range(AXES):
                partial_sum(c, d1, False)
                c_copy(c, d1).start()
            return carry

        lax.fori_loop(0, N_AX - 1, send, 0)
        for c in range(AXES):
            partial_sum(c, 0, True)

        def load(c, d1):
            return pltpu.make_async_copy(cr[c].at[d1 - 1], cv[c].at[d1 - 1], cr_sem.at[c, d1 - 1])

        def store(c):
            off, w = parts[c]
            return pltpu.make_async_copy(yv.at[:, pl.ds(off, w)], y_ref.at[:, pl.ds(off, w)], w_loc.at[c])

        for d1 in (1, 3, 2):
            for c in range(AXES):
                c_copy(c, d1).wait()
                load(c, d1).start()
        for c in range(AXES):
            off, w = parts[c]
            for d1 in (1, 3, 2):
                load(c, d1).wait()
            yv[:, off:off + w] = (acc[:, off:off + w] + cv[c][0] + cv[c][1] + cv[c][2]).astype(BF)
            store(c).start()
        for c in range(AXES):
            store(c).wait()

    pl.run_scoped(combine, pltpu.VMEM((t_loc, d), F32), pltpu.VMEM((t_loc, d), BF), *[pltpu.VMEM((3, t_loc, w), F32) for _, w in parts],
                  *[pltpu.VMEM((3, t_loc, w), F32) for _, w in parts])

    def drain_b(k, carry):
        for c in range(AXES):
            for d2 in range(1, N_AX):
                b_copy(c, k, d2).wait_send()
        return carry

    lax.fori_loop(0, N_AX, drain_b, 0)
    for c in range(AXES):
        for d1 in range(1, N_AX):
            p_copy(c, d1).wait_send()


def _layer(x, idx, g, w1, w3, w2, cap):
    t_loc, d = x.shape
    parts = _parts(d)
    blk = N_AX * cap
    ring_n, st_n = 4, 3
    n_exp = N_AX**AXES
    any_spec = pl.BlockSpec(memory_space=pl.ANY)
    vm = pl.BlockSpec(memory_space=pltpu.VMEM)
    dma = pltpu.SemaphoreType.DMA
    return pl.pallas_call(
        functools.partial(_layer_kernel, parts, cap, ring_n, st_n),
        out_shape=[jax.ShapeDtypeStruct((t_loc, d), BF), jax.ShapeDtypeStruct((n_exp * cap, d), BF)]
        + [jax.ShapeDtypeStruct((3, t_loc, w), F32) for _, w in parts],
        in_specs=[vm, vm, vm] + [any_spec] * 3,
        out_specs=[any_spec] * 5,
        scratch_shapes=[pltpu.VMEM((16, blk, w), BF) for _, w in parts]
        + [pltpu.VMEM((16, blk, w), BF) for _, w in parts]
        + [pltpu.VMEM(w.shape, BF) for w in (w1, w3, w2)]
        + [pltpu.VMEM((3, 16) + idx.shape, jnp.int32), pltpu.VMEM((3, 3, t_loc, 4 * n_exp), BF),
           pltpu.VMEM((t_loc, 4 * n_exp), BF), pltpu.VMEM((t_loc, t_loc), BF),
           dma((3, 16)), dma((3, 16)), dma((3, 16)), dma((3, 16)), dma((3, 16)), dma((3, st_n, 3)), dma((3, 16)),
           dma((3, st_n)), dma((3,)), dma((3,)), dma((3,)), dma((2,)), dma((ring_n, 12)), dma((3, 16)), dma((3, 16)),
           dma((3, 16)), dma((3, 3)), dma((3, 3)), dma((3, 3)), dma((3, 3)), dma((3, 3)), pltpu.SemaphoreType.REGULAR],
        compiler_params=pltpu.CompilerParams(collective_id=0, has_side_effects=True, vmem_limit_bytes=67_043_328),
        name="layer",
    )(x, idx, g, w1, w3, w2)[0]


def solution(mesh):
    ep = mesh.shape["ep"]
    rows = P(("dp", "ep", "tp"), None)

    def local(x, idx, g, w1, w3, w2):
        cap = CF * idx.shape[1] * x.shape[0] // ep
        return _layer(x, idx.T, g.T, w1[0], w3[0], w2[0], cap)

    return jax.shard_map(local, mesh=mesh,
                         in_specs=(rows, rows, rows, P("ep", None, "tp"), P("ep", None, "tp"), P("ep", "tp", None)),
                         out_specs=rows, check_vma=False)
```

```python
import functools

import jax
import jax.numpy as jnp
from jax import lax
from jax.experimental import pallas as pl
from jax.experimental.pallas import tpu as pltpu
from jax.sharding import PartitionSpec as P

CF = 2
N_AX = 4
AXES = 3
VMEM_LIMIT = 60 * 2**20
MESH = pl.DeviceIdType.MESH
BF = jnp.bfloat16
F32 = jnp.float32


def _coords(me):
    return [(me // N_AX**a) % N_AX for a in range(AXES)]


def _shift(m, moves):
    return sum(((m[a] + moves.get(a, 0)) % N_AX) * N_AX**a for a in range(AXES))


def _color(c):
    return (c + 1) % 3, (c + 2) % 3, c


def _greet(m, tp):
    bar = pltpu.get_barrier_semaphore()
    for a in range(AXES):
        for d in range(1, N_AX):
            pl.semaphore_signal(bar, inc=1, device_id={"ep": _shift(m, {a: d})}, device_id_type=MESH)
    pl.semaphore_signal(bar, inc=1, device_id={"tp": 1 - tp}, device_id_type=MESH)


def _meet():
    pl.semaphore_wait(pltpu.get_barrier_semaphore(), AXES * (N_AX - 1) + 1)


def _line(k):
    return k + k // 2 - 2 * (k // 3)


def _split3(v):
    hi = v.astype(BF)
    r = v - hi.astype(F32)
    mid = r.astype(BF)
    return hi, mid, (r - mid.astype(F32)).astype(BF)


def _pack(idx_ref, g_ref, n_exp):
    top, t_loc = idx_ref.shape
    idx, g = idx_ref[...].T, g_ref[...].T
    e = lax.broadcasted_iota(jnp.int32, (t_loc, n_exp), 1)
    member = jnp.zeros((t_loc, n_exp), F32)
    gate = jnp.zeros((t_loc, n_exp), F32)
    for j in range(top):
        hit = idx[:, j:j + 1] == e
        member = jnp.where(hit, 1.0, member)
        gate = jnp.where(hit, g[:, j:j + 1], gate)
    r = lax.broadcasted_iota(jnp.int32, (t_loc, t_loc), 0)
    q = lax.broadcasted_iota(jnp.int32, (t_loc, t_loc), 1)
    lower = jnp.where(q < r, 1.0, 0.0).astype(BF)
    slots = jnp.dot(lower, member.astype(BF), preferred_element_type=F32)
    key = jnp.where(member > 0, slots, -1.0).astype(BF)
    return jnp.concatenate((key,) + _split3(gate), axis=1)


def _far(d):
    return N_AX - d


def _order(k):
    return 1 + 2 * k - 3 * (k // 2)


def _order4(k):
    return (1 + 2 * k - 3 * (k // 2)) % N_AX


def _parts(d):
    return (0, d * 3 // 8), (d * 3 // 8, d * 5 // 16), (d * 11 // 16, d * 5 // 16)


def _layer_kernel(parts, cap, ring_n, st_n, x_ref, idx_ref, g_ref, w1_ref, w3_ref, w2_ref, y_ref, rows_ref, cr0, cr1, cr2,
                  ag0, ag1, ag2, ra0, ra1, ra2, wp1, wp3, wp2, meta, gates_in, packs, mine, tri, *sems):
    (ag_send, ag_send2, ag_recv, mt_send, mt_recv, blk_send, blk_recv, loc_sem, w_send, w_recv, w_loc, x_sem, a_send, a_recv,
     b_send, b_recv, c_send, c_recv, cr_sem, g_send, g_recv, free_sem) = sems
    me, tp = lax.axis_index("ep"), lax.axis_index("tp")
    m = _coords(me)
    ags, ra, cr = (ag0, ag1, ag2), (ra0, ra1, ra2), (cr0, cr1, cr2)
    back, rb = parts, ags
    t_loc, d = x_ref.shape
    n_exp = N_AX**AXES
    half = t_loc // 2
    blk = N_AX * cap
    groups = rows_ref.shape[0] // blk
    _greet(m, tp)

    def remote(src, dst, send, recv, axis, dist):
        return pltpu.make_async_remote_copy(src, dst, send, recv, device_id={"ep": _shift(m, {axis: dist})},
                                            device_id_type=MESH)

    w_refs, w_parts = (w1_ref, w3_ref, w2_ref), (wp1, wp3, wp2)
    w_swaps = [pltpu.make_async_remote_copy(w_refs[i], w_parts[i], w_send.at[i], w_recv.at[i], device_id={"tp": 1 - tp},
                                            device_id_type=MESH) for i in range(3)]


    def whole(c, i_from, i_to, own, axis, dist):
        off, w = parts[c]
        src = x_ref.at[:, pl.ds(off, w)] if own else ags[c].at[i_from]
        return remote(src, ags[c].at[i_to], ag_send.at[c, i_to], ag_recv.at[c, i_to], axis, dist)

    def top(c, i_from, i_to, axis):
        rows = pl.ds(0, half)
        return remote(ags[c].at[i_from, rows], ags[c].at[i_to, rows], ag_send.at[c, i_to], ag_recv.at[c, i_to], axis, 1)

    def bottom(c, i_from, i_to, axis):
        rows = pl.ds(half, half)
        return remote(ags[c].at[i_from, rows], ags[c].at[i_to, rows], ag_send2.at[c, i_to], ag_recv.at[c, i_to], axis, 3)

    def ids_copy(c, i_from, i_to, own, axis, dist):
        src = idx_ref if own else meta.at[c, i_from]
        return remote(src, meta.at[c, i_to], mt_send.at[c, i_to], mt_recv.at[c, i_to], axis, dist)

    def spread(c, i, step, own, axis):
        for dist in (1, 3, 2):
            ids_copy(c, i, i + dist * step, own, axis, dist).start()
        for dist in (1, 3):
            whole(c, i, i + dist * step, own, axis, dist).start()

    def pass_on(c, dist, i, i_to, axis):
        pl.when(dist == 1)(lambda: top(c, i, i_to, axis).start())
        pl.when(dist == 3)(lambda: bottom(c, i, i_to, axis).start())

    def wait_rows(c, i):
        ids_copy(c, i, i, False, 0, 1).wait_recv()
        whole(c, i, i, False, 0, 1).wait_recv()


    def g_copy(c, d1):
        return remote(g_ref, gates_in.at[c, d1 - 1], g_send.at[c, d1 - 1], g_recv.at[c, d1 - 1], _color(c)[0], d1)

    def a_wait(c, i):
        three = ra[c].at[i, pl.ds(0, 3 * cap)]
        pltpu.make_async_copy(three, three, a_recv.at[c, i]).wait()

    def b_copy(c, d1, d2):
        i = d1 * 4 + d2
        return remote(ra[c].at[i], rb[c].at[i], b_send.at[c, i], b_recv.at[c, i], _color(c)[1], _far(d2))

    def forward(k, carry):
        d1, d2 = _order4(k // 4), k % 4
        for c in range(AXES):
            a_wait(c, d1 * 4 + d2)

            @pl.when(d2 > 0)
            def _():
                b_copy(c, d1, d2).start()
        return carry

    def main(st0, st1, st2, wo1, wo3, wo2, xbuf, ring):
        sts, w_own = (st0, st1, st2), (wo1, wo3, wo2)
        w_loads = [pltpu.make_async_copy(w_refs[i], w_own[i], w_loc.at[i]) for i in range(3)]

        def block_copy(c, i, pos, d3):
            off, w = parts[c]
            a1, a2, a3 = _color(c)
            at = [0, 0, 0]
            at[a1], at[a2], at[a3] = i // 4, i % 4, d3
            part = sts[c].at[pos % st_n, pl.ds(d3 * cap, cap)]
            src = at[0] + N_AX * at[1] + N_AX**2 * at[2]
            dst = rows_ref.at[pl.ds(pl.multiple_of(src * cap, cap), cap), pl.ds(off, w)]
            if d3 == 0:
                return pltpu.make_async_copy(part, dst, loc_sem.at[c, pos % st_n])
            return remote(part, dst, blk_send.at[c, pos % st_n, d3 - 1], blk_recv.at[c, at[1] + N_AX * at[2]], a3, d3)

        def pick(c, i, pos, own):
            _, _, a3 = _color(c)
            off, w = parts[c]
            ids = idx_ref[...] if own else meta[c, i]
            member = [jnp.max((ids == _shift(m, {a3: d3})).astype(F32), axis=0, keepdims=True) for d3 in range(N_AX)]
            table = jnp.concatenate(member + [jnp.zeros((4, t_loc), F32)], axis=0)
            slots = jnp.dot(table.astype(BF), tri[...], preferred_element_type=F32)
            key = jnp.where(table > 0, slots, -1.0)
            want = lax.broadcasted_iota(jnp.int32, (cap, t_loc), 0).astype(F32)
            one_hot = jnp.concatenate([jnp.where(key[d3:d3 + 1] == want, 1.0, 0.0) for d3 in range(N_AX)], axis=0)
            one_hot = one_hot.astype(BF)
            for lo in range(0, w, 256):
                hi = min(lo + 256, w)
                xs = x_ref[:, off + lo:off + hi] if own else ags[c][i, :, lo:hi]
                sts[c][pos % st_n, :, lo:hi] = jnp.dot(one_hot, xs, preferred_element_type=F32).astype(BF)

        def local_wait(pos):
            for c in range(AXES):
                block_copy(c, 0, pos, 0).wait()

        def sent_wait(pos):
            for c in range(AXES):
                for d3 in range(1, N_AX):
                    block_copy(c, 0, pos, d3).wait_send()

        def process(i, pos, own=False):
            pl.when(pos >= st_n)(lambda: sent_wait(pos))
            for c in range(AXES):
                pick(c, i, pos, own)
                for d3 in (1, 3, 2, 0):
                    block_copy(c, i, pos, d3).start()
            pl.when(pos >= 1)(lambda: local_wait(pos + st_n - 1))

        r = lax.broadcasted_iota(jnp.int32, (t_loc, t_loc), 0)
        q = lax.broadcasted_iota(jnp.int32, (t_loc, t_loc), 1)
        tri[...] = jnp.where(r < q, 1.0, 0.0).astype(BF)
        for cp in w_loads:
            cp.start()
        _meet()
        for c in range(AXES):
            a1, a2, _ = _color(c)
            spread(c, 0, 4, True, a1)
            spread(c, 0, 1, True, a2)
            for d1 in (1, 3, 2):
                g_copy(c, d1).start()
        for cp in w_swaps:
            cp.start()
        process(0, 0, True)
        mine[...] = _pack(idx_ref, g_ref, n_exp)

        def first_near(k, carry):
            d1 = 1 + 2 * k
            for c in range(AXES):
                a1, a2, _ = _color(c)
                wait_rows(c, d1 * 4)
                pass_on(c, d1, d1 * 4, 8, a1)
                spread(c, d1 * 4, 1, False, a2)
            process(d1 * 4, 1 + k)
            return carry

        def second_near(k, carry):
            d1, d2 = _line(k // 2), 1 + 2 * (k % 2)
            for c in range(AXES):
                wait_rows(c, d1 * 4 + d2)
                pass_on(c, d2, d1 * 4 + d2, d1 * 4 + 2, _color(c)[1])
            process(d1 * 4 + d2, 3 + k + (k + 6) // 8)
            return carry

        def second_far(k, carry):
            d1 = _line(k)
            for c in range(AXES):
                wait_rows(c, d1 * 4 + 2)
            process(d1 * 4 + 2, 12 + k)
            return carry

        lax.fori_loop(0, 2, first_near, 0)
        lax.fori_loop(0, 2, second_near, 0)
        for c in range(AXES):
            wait_rows(c, 8)
            spread(c, 8, 1, False, _color(c)[1])
        process(8, 5)
        lax.fori_loop(2, 8, second_near, 0)

        def group_of(n):
            late = n // 12
            near = n % 3
            return (1 - late) * (near + near // 2) + 2 * late, _line((1 - late) * (n // 3) + late * (n - 12))

        def x_copy(n):
            dy, dz = group_of(n)
            return pltpu.make_async_copy(rows_ref.at[pl.ds((dy + N_AX * dz) * blk, blk)], xbuf.at[n % 2], x_sem.at[n % 2])

        def rows_in(n):
            dy, dz = group_of(n)
            g = dy + N_AX * dz

            def arrived(c, count):
                off, w = parts[c]
                ref = rows_ref.at[pl.ds(g * blk, count * cap), pl.ds(off, w)]
                pltpu.make_async_copy(ref, ref, blk_recv.at[c, g]).wait()

            arrived(0, 3)
            pl.when(dy > 0)(lambda: arrived(1, 4))
            pl.when(dz > 0)(lambda: arrived(2, 4))
            x_copy(n).start()

        def a_each(n, far, near):
            dy, dz = group_of(n)
            for c in range(AXES):
                a1, a2, a3 = _color(c)
                off, w = back[c]
                for dx in range(N_AX):
                    at = (dx, dy, dz)
                    i, d3 = at[a1] * 4 + at[a2], at[a3]

                    def go(c=c, dx=dx, i=i, d3=d3, off=off, w=w, a3=a3):
                        far(remote(ring.at[n % ring_n, pl.ds(dx * cap, cap), pl.ds(off, w)],
                                   ra[c].at[i, pl.ds(d3 * cap, cap)], a_send.at[n % ring_n, c * 4 + dx],
                                   a_recv.at[c, i], a3, _far(d3)))

                    if c == 0:
                        go() if dx else near(c, dx, i)
                    else:
                        pl.when(d3 > 0)(go)
                        pl.when(d3 == 0)(lambda c=c, dx=dx, i=i: near(c, dx, i))

        def step(n, carry):
            x_copy(n).wait()
            pl.when(n + 1 < groups)(lambda: rows_in(n + 1))

            @pl.when(n >= ring_n)
            def _():
                a_each(n - ring_n, lambda cp: cp.wait_send(), lambda c, dx, i: None)

            x = xbuf[n % 2]
            hs = []
            for w1, w3, _ in (w_own, w_parts):
                a = jnp.dot(x, w1[...], preferred_element_type=F32)
                b = jnp.dot(x, w3[...], preferred_element_type=F32)
                hs.append((jax.nn.silu(a) * b).astype(BF))
            for lo in range(0, d, 512):
                y = sum(jnp.dot(h, w[2][:, lo:lo + 512], preferred_element_type=F32) for h, w in zip(hs, (w_own, w_parts)))
                ring[n % ring_n, :, lo:lo + 512] = y.astype(BF)

            def keep(c, dx, i):
                off, w = back[c]
                ra[c][i, 0:cap, :] = ring[n % ring_n, dx * cap:(dx + 1) * cap, off:off + w]

            a_each(n, lambda cp: cp.start(), keep)
            return carry

        for cp in w_loads:
            cp.wait()
        for cp in w_swaps:
            cp.wait_recv()
        def last_rounds(k, carry):
            second_far(k, 0)
            pl.when(k == 1)(lambda: rows_in(0))
            pl.when(k == 3)(lambda: local_wait(15))
            return lax.fori_loop(2 * (k - (k + 3) // 4), 2 * k + 10 * (k // 3), step, carry)

        lax.fori_loop(0, N_AX, last_rounds, 0)

        def drain_far(c, i):
            top(c, i, i, 0).wait_send()
            bottom(c, i, i, 0).wait_send()

        def drain_line(d1, carry):
            for c in range(AXES):
                for d2 in range(1, N_AX):
                    ids_copy(c, 0, d1 * 4 + d2, False, 0, 1).wait_send()
                for d2 in (1, 3):
                    whole(c, 0, d1 * 4 + d2, False, 0, 1).wait_send()
                drain_far(c, d1 * 4 + 2)
            return carry

        lax.fori_loop(0, N_AX, drain_line, 0)
        for c in range(AXES):
            for d1 in range(1, N_AX):
                ids_copy(c, 0, d1 * 4, False, 0, 1).wait_send()
            for d1 in (1, 3):
                whole(c, 0, d1 * 4, False, 0, 1).wait_send()
            drain_far(c, 8)
        for a in range(AXES):
            for dist in range(1, N_AX):
                pl.semaphore_signal(free_sem, inc=1, device_id={"ep": _shift(m, {a: dist})}, device_id_type=MESH)

        pl.semaphore_wait(free_sem, AXES * (N_AX - 1))
        lax.fori_loop(0, groups, forward, 0)

        def unpack(k, carry):
            for c in range(AXES):
                g_copy(c, k + 1).wait_recv()
                packs[c, k] = _pack(meta.at[c, (k + 1) * 4], gates_in.at[c, k], n_exp)
            return carry

        lax.fori_loop(0, N_AX - 1, unpack, 0)

        def drain_ring(n, carry):
            a_each(n, lambda cp: cp.wait_send(), lambda c, dx, i: None)
            return carry

        lax.fori_loop(groups - ring_n, groups, drain_ring, 0)
        for pos in range(16 - st_n, 16):
            sent_wait(pos)
        for cp in w_swaps:
            cp.wait_send()

    weight_scratch = [pltpu.VMEM(w.shape, BF) for w in w_refs]
    pl.run_scoped(main, *[pltpu.VMEM((st_n, blk, w), BF) for _, w in parts], *weight_scratch, pltpu.VMEM((2, blk, d), BF),
                  pltpu.VMEM((ring_n, blk, d), BF))

    def combine(acc, yv, cs0, cs1, cs2, cv0, cv1, cv2):
        cs, cv = (cs0, cs1, cs2), (cv0, cv1, cv2)

        def add_sum(c, d1, d2, own, data):
            _, a2, a3 = _color(c)
            off, w = back[c]
            table = mine[...] if own else packs[c, d1 - 1]
            row = lax.broadcasted_iota(jnp.int32, (N_AX * n_exp, blk), 0)
            col = lax.broadcasted_iota(jnp.int32, (N_AX * n_exp, blk), 1)
            slot = (lax.broadcasted_iota(jnp.int32, (t_loc, blk), 1) % cap).astype(F32)
            e = _shift(m, {a2: d2}) - m[a3] * N_AX**a3 + ((m[a3] + col // cap) % N_AX) * N_AX**a3
            wide = [jnp.where(row == e + n_exp * k, 1.0, 0.0).astype(BF) for k in range(4)]
            hit = jnp.dot(table, wide[0], preferred_element_type=F32) == slot
            gates = [jnp.where(hit, jnp.dot(table, wide[k], preferred_element_type=F32), 0.0).astype(BF) for k in (1, 2, 3)]
            for lo in range(0, w, 256):
                hi = min(lo + 256, w)
                rows = data[:, lo:hi]
                v = sum(jnp.dot(gate, rows, preferred_element_type=F32) for gate in gates)
                at = acc.at[:, off + lo:off + hi] if own else cs[c].at[d1 - 1, :, lo:hi]
                at[...] = v if data_first(d2) else at[...] + v

        def data_first(d2):
            return isinstance(d2, int)

        def partial_sum(c, d1, own):
            add_sum(c, d1, 0, own, ra[c].at[d1 * 4])

            def more(d2, carry):
                b_copy(c, d1, d2).wait_recv()
                add_sum(c, d1, d2, own, rb[c].at[d1 * 4 + d2])
                return carry

            lax.fori_loop(1, N_AX, more, 0)

        def c_copy(c, d1):
            return remote(cs[c].at[d1 - 1], cr[c].at[d1 - 1], c_send.at[c, d1 - 1], c_recv.at[c, d1 - 1], _color(c)[0],
                          _far(d1))

        def load(c, d1):
            return pltpu.make_async_copy(cr[c].at[d1 - 1], cv[c].at[d1 - 1], cr_sem.at[c, d1 - 1])

        def store(c):
            off, w = back[c]
            return pltpu.make_async_copy(yv.at[:, pl.ds(off, w)], y_ref.at[:, pl.ds(off, w)], w_loc.at[c])

        def send(k, carry):
            d1 = _order(k)
            for c in range(AXES):
                partial_sum(c, d1, False)
                c_copy(c, d1).start()
            return carry

        lax.fori_loop(0, N_AX - 1, send, 0)
        for c in range(AXES):
            partial_sum(c, 0, True)
        for d1 in (1, 3, 2):
            for c in range(AXES):
                c_copy(c, d1).wait_recv()
                load(c, d1).start()
        for c in range(AXES):
            off, w = back[c]
            for d1 in (1, 3, 2):
                load(c, d1).wait()
            yv[:, off:off + w] = (acc[:, off:off + w] + cv[c][0] + cv[c][1] + cv[c][2]).astype(BF)
            store(c).start()
        for c in range(AXES):
            store(c).wait()
            for d1 in (1, 3, 2):
                c_copy(c, d1).wait_send()

    pl.run_scoped(combine, pltpu.VMEM((t_loc, d), F32), pltpu.VMEM((t_loc, d), BF), *[pltpu.VMEM((3, t_loc, w), F32) for _, w in back],
                  *[pltpu.VMEM((3, t_loc, w), F32) for _, w in back])

    def drain_b(k, carry):
        for c in range(AXES):
            for d2 in range(1, N_AX):
                b_copy(c, k, d2).wait_send()
        return carry

    lax.fori_loop(0, N_AX, drain_b, 0)
    for c in range(AXES):
        for d1 in range(1, N_AX):
            g_copy(c, d1).wait_send()


def _layer(x, idx, g, w1, w3, w2, cap):
    t_loc, d = x.shape
    parts = _parts(d)
    blk = N_AX * cap
    ring_n, st_n = 4, 3
    n_exp = N_AX**AXES
    any_spec = pl.BlockSpec(memory_space=pl.ANY)
    vm = pl.BlockSpec(memory_space=pltpu.VMEM)
    dma = pltpu.SemaphoreType.DMA
    return pl.pallas_call(
        functools.partial(_layer_kernel, parts, cap, ring_n, st_n),
        out_shape=[jax.ShapeDtypeStruct((t_loc, d), BF), jax.ShapeDtypeStruct((n_exp * cap, d), BF)]
        + [jax.ShapeDtypeStruct((3, t_loc, w), F32) for _, w in parts],
        in_specs=[vm, vm, vm] + [any_spec] * 3,
        out_specs=[any_spec] * 5,
        scratch_shapes=[pltpu.VMEM((16, blk, w), BF) for _, w in parts]
        + [pltpu.VMEM((16, blk, w), BF) for _, w in parts]
        + [pltpu.VMEM(w.shape, BF) for w in (w1, w3, w2)]
        + [pltpu.VMEM((3, 16) + idx.shape, jnp.int32), pltpu.VMEM((3, 3) + g.shape, F32), pltpu.VMEM((3, 3, t_loc, 4 * n_exp), BF),
           pltpu.VMEM((t_loc, 4 * n_exp), BF), pltpu.VMEM((t_loc, t_loc), BF),
           dma((3, 16)), dma((3, 16)), dma((3, 16)), dma((3, 16)), dma((3, 16)), dma((3, st_n, 3)), dma((3, 16)),
           dma((3, st_n)), dma((3,)), dma((3,)), dma((3,)), dma((2,)), dma((ring_n, 12)), dma((3, 16)), dma((3, 16)),
           dma((3, 16)), dma((3, 3)), dma((3, 3)), dma((3, 3)), dma((3, 3)), dma((3, 3)), pltpu.SemaphoreType.REGULAR],
        compiler_params=pltpu.CompilerParams(collective_id=0, has_side_effects=True, vmem_limit_bytes=67_043_328),
        name="layer",
    )(x, idx, g, w1, w3, w2)[0]


def solution(mesh):
    ep = mesh.shape["ep"]
    rows = P(("dp", "ep", "tp"), None)

    def local(x, idx, g, w1, w3, w2):
        cap = CF * idx.shape[1] * x.shape[0] // ep
        return _layer(x, idx.T, g.T, w1[0], w3[0], w2[0], cap)

    return jax.shard_map(local, mesh=mesh,
                         in_specs=(rows, rows, rows, P("ep", None, "tp"), P("ep", None, "tp"), P("ep", "tp", None)),
                         out_specs=rows, check_vma=False)
```
